32 devices in a mesh: row: 8 (over z, core), col: 4 (over y, x).
Axes of the slice: x: 2, y: 2, z: 4, core: 2. Of those that a mesh axis runs over, the one named last changes fastest.
Arguments:
- substrate: float32 [1024, 1024], P('row', 'col'), may hold values from 0.05 to 0.95
- activator: float32 [1024, 1024], P('row', 'col'), may hold values from 0 to 0.45
Outputs:
- substrate_section: float32 [1024, 1024], P('row', 'col')
- activator_section: float32 [1024, 1024], P('row', 'col')
The draws below stay inside these ranges and needn't reach their ends.
All inputs are finite; a program needn't handle non-finite values.
Results may differ from the reference program's by a relative error of at most 0.00023.
Values sent between devices are 32-bit elements; how exact they have to be, the bound alone decides.
A program may use at most 64 MiB of HBM per device.

```python
import math
import jax
import jax.numpy as jnp

NX = 1024
NY = 1024


def smooth_part(key):
    orders = jnp.arange(1, 5, dtype=jnp.float32)
    row_coords = jnp.arange(NX, dtype=jnp.float32) / NX
    col_coords = jnp.arange(NY, dtype=jnp.float32) / NY
    row_angles = 2.0 * math.pi * orders[:, None] * row_coords[None, :]
    col_angles = 2.0 * math.pi * orders[:, None] * col_coords[None, :]
    basis_rows = jnp.concatenate([jnp.cos(row_angles), jnp.sin(row_angles)], axis=0)
    basis_cols = jnp.concatenate([jnp.cos(col_angles), jnp.sin(col_angles)], axis=0)
    coefficients = jax.random.normal(key, (8, 8), jnp.float32)
    mixed = jnp.dot(coefficients, basis_cols, preferred_element_type=jnp.float32)
    return jnp.dot(basis_rows.T, mixed, preferred_element_type=jnp.float32) / 4.0


def draw_substrate(key, part):
    smooth = smooth_part(jax.random.fold_in(key, 11))
    rough_key = jax.random.fold_in(key, 12)
    rough_part = jax.random.uniform(rough_key, (NX, NY), jnp.float32, -1.0, 1.0)
    return (0.55 + 0.2 * jnp.tanh(smooth) + 0.15 * rough_part).astype(jnp.float32)


def draw_activator(key, part):
    smooth = smooth_part(jax.random.fold_in(key, 23))
    rough_key = jax.random.fold_in(key, 24)
    rough_part = jax.random.uniform(rough_key, (NX, NY), jnp.float32, -1.0, 1.0)
    return (0.25 + 0.08 * jnp.tanh(smooth) + 0.08 * rough_part).astype(jnp.float32)


def setup_inputs(seed: int = 0) -> dict:
    key_of = jax.random.split(jax.random.key(seed), 3)
    substrate = draw_substrate(jax.random.fold_in(key_of[2], 71), 0)
    activator = draw_activator(jax.random.fold_in(key_of[2], 71), 0)
    return dict(substrate=substrate, activator=activator)


FEED_RATE = 0.037
KILL_RATE = 0.06
TIME_STEP = 8.0
SUBSTRATE_DIFFUSION = 4e-7
ACTIVATOR_DIFFUSION = 2e-7


def signed_squares(total):
    indices = jnp.arange(total, dtype=jnp.int32)
    signed = jnp.where(2 * indices < total, indices, indices - total).astype(jnp.float32)
    angular = (2.0 * math.pi) * signed
    return angular * angular


def section_factors(wave_number, diffusion, decay_rate):
    linear = -diffusion * wave_number - decay_rate
    exponent = linear * (0.5 * TIME_STEP)
    return jnp.exp(exponent), jnp.expm1(exponent) / linear


def species_section(field, source, wave_number, diffusion, decay_rate):
    growth, forcing = section_factors(wave_number, diffusion, decay_rate)
    spectrum = jnp.fft.fft2(field + 1j * source)
    advanced = spectrum * (growth - 1j * forcing)
    return jnp.real(jnp.fft.ifft2(advanced)).astype(jnp.float32)


def reference(substrate, activator):
    reaction = substrate * activator * activator
    wave_number = signed_squares(NX)[:, None] + signed_squares(NY)[None, :]
    substrate_section = species_section(substrate, FEED_RATE - reaction, wave_number, SUBSTRATE_DIFFUSION, FEED_RATE)
    activator_section = species_section(activator, reaction, wave_number, ACTIVATOR_DIFFUSION, FEED_RATE + KILL_RATE)
    return (substrate_section, activator_section)
```

```python
import functools
import math

import jax
import jax.numpy as jnp
import numpy as np
from jax import lax
from jax.experimental import pallas as pl
from jax.experimental.pallas import tpu as pltpu
from jax.sharding import PartitionSpec as P

FEED_RATE = 0.037
KILL_RATE = 0.06
TIME_STEP = 8.0
SUBSTRATE_DIFFUSION = 4e-07
ACTIVATOR_DIFFUSION = 2e-07


def rotation(left_index, right_index, period, direction):
    phase_index = left_index * right_index % period
    angles = phase_index.astype(jnp.float32) * (2.0 * math.pi / period)
    return (jnp.cos(angles), direction * jnp.sin(angles))


def complex_matrix(size_count, direction):
    indices = jnp.arange(size_count, dtype=jnp.int32)
    cosine_part, sine_part = rotation(indices[:, None], indices[None, :], size_count, direction)
    return jnp.stack([jnp.stack([cosine_part, -sine_part]), jnp.stack([sine_part, cosine_part])])


def transform_last(values, direction):
    part_count, species, middle, length = values.shape
    leading = 64
    second = length // leading
    shaped = values.reshape(part_count, species, middle, leading, second)
    first_matrix = complex_matrix(leading, direction)
    first_pass = jnp.einsum(
        "pqka,qsmab->psmkb", first_matrix, shaped, precision=lax.Precision.HIGHEST
    )
    cosine_part, sine_part = rotation(
        jnp.arange(leading, dtype=jnp.int32)[:, None],
        jnp.arange(second, dtype=jnp.int32)[None, :],
        length,
        direction,
    )
    turned = jnp.stack(
        [
            first_pass[0] * cosine_part - first_pass[1] * sine_part,
            first_pass[0] * sine_part + first_pass[1] * cosine_part,
        ]
    )
    second_matrix = complex_matrix(second, direction)
    second_pass = jnp.einsum(
        "pqkb,qsmjb->psmkj", second_matrix, turned, precision=lax.Precision.HIGHEST
    )
    return second_pass.reshape(part_count, species, middle, length)


def signed_squares(wave_index, total):
    signed = jnp.where(2 * wave_index < total, wave_index, wave_index - total).astype(jnp.float32)
    angular = 2.0 * math.pi * signed
    return angular * angular


def section_factors(row_wave, col_wave, total_rows, total_cols):
    wave_number = signed_squares(row_wave, total_rows) + signed_squares(col_wave, total_cols)
    normalize = 1.0 / (total_rows * total_cols)
    growths = []
    forcings = []
    for diffusion, decay_rate in (
        (SUBSTRATE_DIFFUSION, FEED_RATE),
        (ACTIVATOR_DIFFUSION, FEED_RATE + KILL_RATE),
    ):
        linear = -diffusion * wave_number - decay_rate
        exponent = linear * (0.5 * TIME_STEP)
        growths.append(jnp.exp(exponent) * normalize)
        forcings.append(jnp.expm1(exponent) / linear * normalize)
    return (jnp.stack(growths), jnp.stack(forcings))


def advance(spectra, growth, forcing):
    real_part = spectra[0]
    imag_part = spectra[1]
    return jnp.stack(
        [growth * real_part + forcing * imag_part, growth * imag_part - forcing * real_part]
    )


def col_forward(values):
    return lax.all_to_all(values, "col", split_axis=2, concat_axis=3, tiled=True)


def col_backward(values):
    return lax.all_to_all(values, "col", split_axis=3, concat_axis=2, tiled=True)


def row_forward(values):
    return lax.all_to_all(values, "row", split_axis=2, concat_axis=3, tiled=True)


def row_backward(values):
    return lax.all_to_all(values, "row", split_axis=3, concat_axis=2, tiled=True)


def on_device(substrate, activator):
    row_count, col_count = substrate.shape
    total_rows = row_count * lax.axis_size("row")
    total_cols = col_count * lax.axis_size("col")
    row_index = lax.axis_index("row")
    col_index = lax.axis_index("col")
    reaction = substrate * activator * activator
    fields = jnp.stack(
        [jnp.stack([substrate, activator]), jnp.stack([FEED_RATE - reaction, reaction])]
    )
    spectra = transform_last(col_forward(fields), -1)
    spectra = row_forward(col_forward(jnp.swapaxes(spectra, 2, 3)))
    spectra = transform_last(spectra, -1)
    local_cols = col_count // lax.axis_size("row")
    col_wave = (
        col_count * col_index
        + local_cols * row_index
        + jnp.arange(local_cols, dtype=jnp.int32)[:, None]
    )
    row_wave = jnp.arange(total_rows, dtype=jnp.int32)[None, :]
    growth, forcing = section_factors(row_wave, col_wave, total_rows, total_cols)
    spectra = transform_last(advance(spectra, growth, forcing), 1)
    spectra = col_backward(row_backward(spectra))
    spectra = jnp.swapaxes(spectra, 2, 3)
    spectra = transform_last(spectra, 1)
    fields = lax.all_to_all(spectra[:1], "col", split_axis=3, concat_axis=2, tiled=True)
    return (fields[0, 0], fields[0, 1])


MESH = pl.DeviceIdType.MESH
LANES = 128


def split(values):
    high = values.astype(jnp.bfloat16)
    low = (values - high.astype(jnp.float32)).astype(jnp.bfloat16)
    return high, low


def contract_last(left, right):
    return lax.dot_general(
        left, right, (((1,), (1,)), ((), ())), preferred_element_type=jnp.float32
    )


def block_transpose(pieces):
    first, second, third, fourth = pieces
    lane = lax.broadcasted_iota(jnp.int32, first.shape, 1)
    upper = lane < LANES // 2
    even = lane // (LANES // 4) % 2 == 0

    def far(a, b):
        return (
            jnp.where(upper, a, pltpu.roll(b, LANES // 2, 1)),
            jnp.where(upper, pltpu.roll(a, LANES // 2, 1), b),
        )

    def near(a, b):
        return (
            jnp.where(even, a, pltpu.roll(b, LANES // 4, 1)),
            jnp.where(even, pltpu.roll(a, 3 * LANES // 4, 1), b),
        )

    first, third = far(first, third)
    second, fourth = far(second, fourth)
    first, second = near(first, second)
    third, fourth = near(third, fourth)
    return first, second, third, fourth


def section_kernel(
    rows, cols, u_hbm, v_hbm, tables_hbm, sections, u_ref, v_ref, tables_ref,
    c_high, c_low, x_in, packed, wide, send, recv, result,
    ready, load_sem, in_send, in_recv, s_send, s_recv, out_send, out_recv,
):
    devices = rows * cols
    total = u_ref.shape[1] * cols
    band = u_ref.shape[0] // cols
    width = u_ref.shape[1]
    chunk = 256
    row = lax.axis_index("row")
    col = lax.axis_index("col")
    me = row * cols + col

    loads = [
        pltpu.make_async_copy(source, target, load_sem.at[index])
        for index, (source, target) in enumerate(
            ((u_hbm, u_ref), (v_hbm, v_ref), (tables_hbm, tables_ref))
        )
    ]
    for load in loads:
        load.start()
    barrier = pltpu.get_barrier_semaphore()

    def greet(semaphore, other_row, other_col):
        pl.semaphore_signal(
            semaphore, inc=1, device_id=(other_row, other_col), device_id_type=MESH
        )

    for step in range(1, cols):
        greet(barrier, row, lax.rem(col + step, cols))
    for step in range(1, rows):
        greet(barrier, lax.rem(row + step, rows), col)
    for load in loads[:2]:
        load.wait()
    pl.semaphore_wait(barrier, rows + cols - 2)

    def in_copy(step, field):
        ref = (u_ref, v_ref)[field]
        other = lax.rem(col + step, cols)
        return pltpu.make_async_remote_copy(
            src_ref=ref.at[pl.ds(pl.multiple_of(other * band, band), band)],
            dst_ref=x_in.at[field, col],
            send_sem=in_send.at[field, step],
            recv_sem=in_recv.at[field, step],
            device_id=(row, other),
            device_id_type=MESH,
        )

    in_copies = [[in_copy(step, field) for step in range(1, cols)] for field in range(2)]
    for copy in in_copies[1] + in_copies[0]:
        copy.start()
    for step in range(1, rows):
        greet(ready, lax.rem(row + step, rows), col)
    for field, ref in enumerate((u_ref, v_ref)):
        x_in[field, col] = ref[pl.ds(pl.multiple_of(col * band, band), band)]

    group = tables_ref.shape[1]
    loads[2].wait()

    def build(step, carry):
        cosine = tables_ref[0, pl.ds(step, 1)]
        sine = tables_ref[1, pl.ds(step, 1)]
        high, low = split(cosine * tables_ref[2] + sine * tables_ref[3])
        at = pl.ds(pl.multiple_of(step * group, group), group)
        c_high[at] = high
        c_low[at] = low
        return carry

    lax.fori_loop(0, total // group, build, 0)

    def filters():
        shape = (band, total)
        q = me * band + lax.broadcasted_iota(jnp.int32, shape, 0)
        p = lax.broadcasted_iota(jnp.int32, shape, 1)
        wave_number = signed_squares(p, total) + signed_squares(q, total)
        growths, forcings = [], []
        for diffusion, decay_rate in (
            (SUBSTRATE_DIFFUSION, FEED_RATE),
            (ACTIVATOR_DIFFUSION, FEED_RATE + KILL_RATE),
        ):
            linear = -diffusion * wave_number - decay_rate
            growth = jnp.exp(linear * (0.5 * TIME_STEP))
            growths.append(growth)
            forcings.append((growth - 1.0) / linear)
        return growths, forcings

    quarter = band // 4
    per_chunk = chunk // band
    chunks = total // chunk

    def remote(leg, other):
        step = lax.rem(other - me + devices, devices)
        return pltpu.make_async_remote_copy(
            src_ref=send.at[leg, other],
            dst_ref=recv.at[leg, me],
            send_sem=s_send.at[leg, step],
            recv_sem=s_recv.at[leg, step],
            device_id=(other // cols, lax.rem(other, cols)),
            device_id_type=MESH,
        )

    def spread(field):
        high, low = split(field)
        for copy_at in range(4):
            wide[copy_at * band : (copy_at + 1) * band] = high
            wide[(4 + copy_at) * band : (5 + copy_at) * band] = low

    def launch(leg):
        lane = lax.broadcasted_iota(jnp.int32, (per_chunk, quarter, LANES), 2) // (LANES // 4)

        def body(step, carry):
            number = lax.rem(row * chunks // rows + chunks // 2 + step, chunks)
            at = pl.ds(pl.multiple_of(number * chunk, chunk), chunk)
            both = contract_last(c_high[at], wide[...])
            out = both[:, :LANES] + both[:, LANES:] + contract_last(c_low[at], wide[:LANES])
            out = out.reshape(per_chunk, band, LANES)
            first = number * per_chunk
            piece = out[:, :quarter]
            for j in range(1, 4):
                piece = jnp.where(lane == j, out[:, j * quarter : (j + 1) * quarter], piece)
            send[leg, pl.ds(first, per_chunk)] = piece

            def start(index, carry):
                other = first + index

                @pl.when(other != me)
                def _():
                    remote(leg, other).start()

                return carry

            return lax.fori_loop(0, per_chunk, start, carry)

        lax.fori_loop(0, chunks, body, 0)
        recv[leg, me] = send[leg, me]

    def land(leg):
        def wait(step, carry):
            remote(leg, lax.rem(me + step, devices)).wait_recv()
            return carry

        lax.fori_loop(1, devices, wait, 0)
        for g in range(devices // 4):
            pieces = block_transpose([recv[leg, 4 * g + k] for k in range(4)])
            at = slice(g * LANES, (g + 1) * LANES)
            for j in range(4):
                high, low = split(pieces[j])
                packed[j * quarter : (j + 1) * quarter, at] = high.astype(jnp.float32)
                packed[band + j * quarter : band + (j + 1) * quarter, at] = low.astype(
                    jnp.float32
                )
        both = packed[...].astype(jnp.bfloat16)
        out = []
        for number in range(chunks):
            at = slice(number * chunk, (number + 1) * chunk)
            dot = functools.partial(jnp.dot, preferred_element_type=jnp.float32)
            product = dot(both, c_high[:, at])
            out.append(product[:band] + product[band:] + dot(both[:band], c_low[:, at]))
        return out

    def gathered(field):
        for copy in in_copies[field]:
            copy.wait_recv()
        return jnp.concatenate([x_in[field, block] for block in range(cols)], axis=1)

    v = gathered(1)
    spread(v)
    pl.semaphore_wait(ready, rows - 1)
    launch(0)
    u = gathered(0)
    v = jnp.concatenate([x_in[1, block] for block in range(cols)], axis=1)
    spread(u * v * v)
    launch(1)
    spread(jnp.concatenate([x_in[0, block] for block in range(cols)], axis=1))
    launch(2)
    growth, forcing = filters()
    activator = growth[1] * jnp.concatenate(land(0), axis=1)
    reaction = jnp.concatenate(land(1), axis=1)
    spread(activator + forcing[1] * reaction)
    launch(3)
    reaction = forcing[0] * reaction
    spread(growth[0] * jnp.concatenate(land(2), axis=1) - reaction)
    launch(4)

    def out_copy(step, field):
        ref = sections.at[field]
        other = lax.rem(col + step, cols)
        return pltpu.make_async_remote_copy(
            src_ref=result.at[field, other],
            dst_ref=ref.at[pl.ds(pl.multiple_of(col * band, band), band)],
            send_sem=out_send.at[field, step],
            recv_sem=out_recv.at[field, step],
            device_id=(row, other),
            device_id_type=MESH,
        )

    out_copies = []
    for leg, field in ((3, 1), (4, 0)):
        for number, out in enumerate(land(leg)):
            result[field, number] = out
        for step in range(1, cols):
            out_copies.append(out_copy(step, field))
            out_copies[-1].start()
        sections[field, pl.ds(pl.multiple_of(col * band, band), band)] = result[field, col]
    for copy in in_copies[0] + in_copies[1]:
        copy.wait_send()

    def drain(step, carry):
        for leg in range(5):
            remote(leg, lax.rem(me + step, devices)).wait_send()
        return carry

    lax.fori_loop(1, devices, drain, 0)
    for copy in out_copies:
        copy.wait()


def tables(total, group):
    wave = np.arange(total)

    def angles(index):
        return 2.0 * np.pi / total * (index[:, None] * wave[None, :] % total)

    coarse = angles(np.arange(total // group) * group)
    fine = angles(np.arange(group))
    return jnp.asarray(
        np.stack(
            (
                np.cos(coarse),
                np.sin(coarse),
                np.cos(fine) + np.sin(fine),
                np.cos(fine) - np.sin(fine),
            )
        ),
        jnp.float32,
    )


def on_device_fused(rows, cols, substrate, activator):
    height, width = substrate.shape
    total = width * cols
    band = height // cols
    devices = rows * cols
    bf16, f32 = jnp.bfloat16, jnp.float32
    dma = pltpu.SemaphoreType.DMA
    vmem = pl.BlockSpec(memory_space=pltpu.VMEM)
    operands = (substrate, activator, tables(total, 32))
    sections = pl.pallas_call(
        functools.partial(section_kernel, rows, cols),
        out_shape=jax.ShapeDtypeStruct((2,) + substrate.shape, f32),
        in_specs=[pl.BlockSpec(memory_space=pltpu.HBM)] * 3,
        out_specs=vmem,
        scratch_shapes=[
            pltpu.VMEM(substrate.shape, f32),
            pltpu.VMEM(substrate.shape, f32),
            pltpu.VMEM((4, 32, total), f32),
            pltpu.VMEM((total, total), bf16),
            pltpu.VMEM((total, total), bf16),
            pltpu.VMEM((2, cols, band, width), f32),
            pltpu.VMEM((2 * band, total), f32),
            pltpu.VMEM((8 * band, total), bf16),
            pltpu.VMEM((5, devices, band // 4, LANES), f32),
            pltpu.VMEM((5, devices, band // 4, LANES), f32),
            pltpu.VMEM((2, cols, band, width), f32),
            pltpu.SemaphoreType.REGULAR,
            dma((3,)),
            dma((2, cols)),
            dma((2, cols)),
            dma((5, devices)),
            dma((5, devices)),
            dma((2, cols)),
            dma((2, cols)),
        ],
        compiler_params=pltpu.CompilerParams(
            collective_id=0, has_side_effects=True, vmem_limit_bytes=48 * 2**20
        ),
    )(*(pltpu.with_memory_space_constraint(value, pltpu.HBM) for value in operands))
    zero = -(FEED_RATE)
    constant = FEED_RATE * math.expm1(zero * 0.5 * TIME_STEP) / zero
    normalize = 1.0 / (total * total)
    return sections[0] * normalize + constant, sections[1] * normalize


def dispatch(rows, cols, substrate, activator):
    height, width = substrate.shape
    total = width * cols
    band = height // cols
    dense_fits = total * total * 4 <= 16 * 2**20
    fits = height * rows == total and 4 * band == LANES and band * rows * cols == total
    if fits and dense_fits and width == 256:
        return on_device_fused(rows, cols, substrate, activator)
    return on_device(substrate, activator)


def solution(mesh):
    in_specs = (P("row", "col"), P("row", "col"))
    out_specs = (P("row", "col"), P("row", "col"))
    return jax.shard_map(
        functools.partial(dispatch, mesh.shape["row"], mesh.shape["col"]),
        mesh=mesh,
        in_specs=in_specs,
        out_specs=out_specs,
        check_vma=False,
    )
```

```python
import functools
import math

import jax
import jax.numpy as jnp
import numpy as np
from jax import lax
from jax.experimental import pallas as pl
from jax.experimental.pallas import tpu as pltpu
from jax.sharding import PartitionSpec as P

FEED_RATE = 0.037
KILL_RATE = 0.06
TIME_STEP = 8.0
SUBSTRATE_DIFFUSION = 4e-07
ACTIVATOR_DIFFUSION = 2e-07


def rotation(left_index, right_index, period, direction):
    phase_index = left_index * right_index % period
    angles = phase_index.astype(jnp.float32) * (2.0 * math.pi / period)
    return (jnp.cos(angles), direction * jnp.sin(angles))


def complex_matrix(size_count, direction):
    indices = jnp.arange(size_count, dtype=jnp.int32)
    cosine_part, sine_part = rotation(indices[:, None], indices[None, :], size_count, direction)
    return jnp.stack([jnp.stack([cosine_part, -sine_part]), jnp.stack([sine_part, cosine_part])])


def transform_last(values, direction):
    part_count, species, middle, length = values.shape
    leading = 64
    second = length // leading
    shaped = values.reshape(part_count, species, middle, leading, second)
    first_matrix = complex_matrix(leading, direction)
    first_pass = jnp.einsum(
        "pqka,qsmab->psmkb", first_matrix, shaped, precision=lax.Precision.HIGHEST
    )
    cosine_part, sine_part = rotation(
        jnp.arange(leading, dtype=jnp.int32)[:, None],
        jnp.arange(second, dtype=jnp.int32)[None, :],
        length,
        direction,
    )
    turned = jnp.stack(
        [
            first_pass[0] * cosine_part - first_pass[1] * sine_part,
            first_pass[0] * sine_part + first_pass[1] * cosine_part,
        ]
    )
    second_matrix = complex_matrix(second, direction)
    second_pass = jnp.einsum(
        "pqkb,qsmjb->psmkj", second_matrix, turned, precision=lax.Precision.HIGHEST
    )
    return second_pass.reshape(part_count, species, middle, length)


def signed_squares(wave_index, total):
    signed = jnp.where(2 * wave_index < total, wave_index, wave_index - total).astype(jnp.float32)
    angular = 2.0 * math.pi * signed
    return angular * angular


def section_factors(row_wave, col_wave, total_rows, total_cols):
    wave_number = signed_squares(row_wave, total_rows) + signed_squares(col_wave, total_cols)
    normalize = 1.0 / (total_rows * total_cols)
    growths = []
    forcings = []
    for diffusion, decay_rate in (
        (SUBSTRATE_DIFFUSION, FEED_RATE),
        (ACTIVATOR_DIFFUSION, FEED_RATE + KILL_RATE),
    ):
        linear = -diffusion * wave_number - decay_rate
        exponent = linear * (0.5 * TIME_STEP)
        growths.append(jnp.exp(exponent) * normalize)
        forcings.append(jnp.expm1(exponent) / linear * normalize)
    return (jnp.stack(growths), jnp.stack(forcings))


def advance(spectra, growth, forcing):
    real_part = spectra[0]
    imag_part = spectra[1]
    return jnp.stack(
        [growth * real_part + forcing * imag_part, growth * imag_part - forcing * real_part]
    )


def col_forward(values):
    return lax.all_to_all(values, "col", split_axis=2, concat_axis=3, tiled=True)


def col_backward(values):
    return lax.all_to_all(values, "col", split_axis=3, concat_axis=2, tiled=True)


def row_forward(values):
    return lax.all_to_all(values, "row", split_axis=2, concat_axis=3, tiled=True)


def row_backward(values):
    return lax.all_to_all(values, "row", split_axis=3, concat_axis=2, tiled=True)


def on_device(substrate, activator):
    row_count, col_count = substrate.shape
    total_rows = row_count * lax.axis_size("row")
    total_cols = col_count * lax.axis_size("col")
    row_index = lax.axis_index("row")
    col_index = lax.axis_index("col")
    reaction = substrate * activator * activator
    fields = jnp.stack(
        [jnp.stack([substrate, activator]), jnp.stack([FEED_RATE - reaction, reaction])]
    )
    spectra = transform_last(col_forward(fields), -1)
    spectra = row_forward(col_forward(jnp.swapaxes(spectra, 2, 3)))
    spectra = transform_last(spectra, -1)
    local_cols = col_count // lax.axis_size("row")
    col_wave = (
        col_count * col_index
        + local_cols * row_index
        + jnp.arange(local_cols, dtype=jnp.int32)[:, None]
    )
    row_wave = jnp.arange(total_rows, dtype=jnp.int32)[None, :]
    growth, forcing = section_factors(row_wave, col_wave, total_rows, total_cols)
    spectra = transform_last(advance(spectra, growth, forcing), 1)
    spectra = col_backward(row_backward(spectra))
    spectra = jnp.swapaxes(spectra, 2, 3)
    spectra = transform_last(spectra, 1)
    fields = lax.all_to_all(spectra[:1], "col", split_axis=3, concat_axis=2, tiled=True)
    return (fields[0, 0], fields[0, 1])


MESH = pl.DeviceIdType.MESH
LANES = 128


def split(values):
    high = values.astype(jnp.bfloat16)
    low = (values - high.astype(jnp.float32)).astype(jnp.bfloat16)
    return high, low


def contract_last(left, right):
    return lax.dot_general(
        left, right, (((1,), (1,)), ((), ())), preferred_element_type=jnp.float32
    )


def block_transpose(pieces):
    first, second, third, fourth = pieces
    lane = lax.broadcasted_iota(jnp.int32, first.shape, 1)
    upper = lane < LANES // 2
    even = lane // (LANES // 4) % 2 == 0

    def far(a, b):
        return (
            jnp.where(upper, a, pltpu.roll(b, LANES // 2, 1)),
            jnp.where(upper, pltpu.roll(a, LANES // 2, 1), b),
        )

    def near(a, b):
        return (
            jnp.where(even, a, pltpu.roll(b, LANES // 4, 1)),
            jnp.where(even, pltpu.roll(a, 3 * LANES // 4, 1), b),
        )

    first, third = far(first, third)
    second, fourth = far(second, fourth)
    first, second = near(first, second)
    third, fourth = near(third, fourth)
    return first, second, third, fourth


def section_kernel(
    rows, cols, u_hbm, v_hbm, tables_hbm, sections, u_ref, v_ref, tables_ref,
    forth, flipped, x_in, packed, wide, filters, spectrum, send, recv, result,
    ready, load_sem, in_send, in_recv, s_send, s_recv, out_send, out_recv,
):
    devices = rows * cols
    total = u_ref.shape[1] * cols
    half = total // 2
    band = u_ref.shape[0] // cols
    quarter = band // 4
    chunk = half // 2
    group = 32
    row = lax.axis_index("row")
    col = lax.axis_index("col")
    me = row * cols + col

    loads = [
        pltpu.make_async_copy(source, target, load_sem.at[index])
        for index, (source, target) in enumerate(
            ((v_hbm, v_ref), (u_hbm, u_ref), (tables_hbm, tables_ref))
        )
    ]
    for load in loads:
        load.start()
    barrier = pltpu.get_barrier_semaphore()

    def greet(semaphore, other_row, other_col):
        pl.semaphore_signal(
            semaphore, inc=1, device_id=(other_row, other_col), device_id_type=MESH
        )

    for step in range(1, cols):
        greet(barrier, row, lax.rem(col + step, cols))
    for step in range(1, rows):
        greet(barrier, lax.rem(row + step, rows), col)
    for load in loads[:2]:
        load.wait()
    pl.semaphore_wait(barrier, rows + cols - 2)

    def in_copy(step, field):
        ref = (u_ref, v_ref)[field]
        other = lax.rem(col + step, cols)
        return pltpu.make_async_remote_copy(
            src_ref=ref.at[pl.ds(pl.multiple_of(other * band, band), band)],
            dst_ref=x_in.at[field, col],
            send_sem=in_send.at[field, step],
            recv_sem=in_recv.at[field, step],
            device_id=(row, other),
            device_id_type=MESH,
        )

    in_copies = [[in_copy(step, field) for step in range(1, cols)] for field in range(2)]
    for copy in in_copies[1] + in_copies[0]:
        copy.start()
    for step in range(1, rows):
        greet(ready, lax.rem(row + step, rows), col)
    for field, ref in enumerate((u_ref, v_ref)):
        x_in[field, col] = ref[pl.ds(pl.multiple_of(col * band, band), band)]
    loads[2].wait()

    def build(target, coarse, fine):
        def body(step, carry):
            cosine = tables_ref[6 + coarse, pl.ds(step, 1)]
            sine = tables_ref[7 + coarse, pl.ds(step, 1)]
            high, low = split(cosine * tables_ref[fine] + sine * tables_ref[fine + 1])
            at = pl.ds(pl.multiple_of(step * group, group), group)
            target[0, at] = high
            target[1, at] = low
            return carry

        lax.fori_loop(0, half // group, body, 0)

    build(forth.at[0], 0, 0)
    build(forth.at[1], 0, 2)

    def wave(position):
        return jnp.where(position < half, 2 * position, 2 * (position - half) + 1)

    def fill_filters():
        shape = (band, total)
        q = wave(me * band + lax.broadcasted_iota(jnp.int32, shape, 0))
        p = wave(lax.broadcasted_iota(jnp.int32, shape, 1))
        wave_number = signed_squares(p, total) + signed_squares(q, total)
        for index, (diffusion, decay_rate) in enumerate((
            (SUBSTRATE_DIFFUSION, FEED_RATE),
            (ACTIVATOR_DIFFUSION, FEED_RATE + KILL_RATE),
        )):
            linear = -diffusion * wave_number - decay_rate
            growth = jnp.exp(linear * (0.5 * TIME_STEP))
            filters[2 * index] = growth
            filters[2 * index + 1] = (growth - 1.0) / linear

    def remote(leg, other):
        return pltpu.make_async_remote_copy(
            src_ref=send.at[leg, other],
            dst_ref=recv.at[leg, me],
            send_sem=s_send.at[leg],
            recv_sem=s_recv.at[leg],
            device_id=(other // cols, lax.rem(other, cols)),
            device_id_type=MESH,
        )

    def all_of(leg):
        others = pl.ds(0, devices - 1)
        other = lax.rem(me + 1, devices)
        return pltpu.make_async_remote_copy(
            src_ref=send.at[leg, others],
            dst_ref=recv.at[leg, others],
            send_sem=s_send.at[leg],
            recv_sem=s_recv.at[leg],
            device_id=(other // cols, lax.rem(other, cols)),
            device_id_type=MESH,
        )

    def spread(parity, field):
        high, low = split(field)
        for copy_at in range(4):
            wide[parity, copy_at * band : (copy_at + 1) * band] = high
            wide[parity, (4 + copy_at) * band : (5 + copy_at) * band] = low

    def product(high, low, parity):
        both = contract_last(high, wide[parity])
        return both[:, :LANES] + both[:, LANES:] + contract_last(low, wide[parity, :LANES])

    def stage(leg, first, values):
        count = values.shape[0] // band
        lane = lax.broadcasted_iota(jnp.int32, (count, quarter, LANES), 2) // (LANES // 4)
        out = values.reshape(count, band, LANES)
        piece = out[:, :quarter]
        for j in range(1, 4):
            piece = jnp.where(lane == j, out[:, j * quarter : (j + 1) * quarter], piece)
        send[leg, pl.ds(first, count)] = piece


    def begin(leg, other):
        remote(leg, other).start()

    def forward(leg):
        count = devices // 2
        mine = me // count
        for step in range(2):
            parity = lax.rem(mine + 1 + step, 2)
            stage(leg, parity * count, product(forth[parity, 0], forth[parity, 1], parity))
            for k in range(step, count):
                begin(leg, parity * count + lax.rem(me + k, count))
        recv[leg, me] = send[leg, me]

    def inverse(leg):
        count = devices // 4
        side = me // (2 * count)
        mine = lax.rem(me, 2 * count) // count
        for step in range(2):
            part = lax.rem(mine + 1 + step, 2)
            at = pl.ds(pl.multiple_of(part * chunk, chunk), chunk)
            first = product(forth[0, 0, at], forth[0, 1, at], 0)
            second = product(flipped[0, at], flipped[1, at], 1)
            stage(leg, part * count, first + second)
            stage(leg, part * count + 2 * count, first - second)
            for k in range(count):
                other = part * count + lax.rem(me + k, count)
                begin(leg, other + 2 * count * (1 - side))
                if step == 0 or k > 0:
                    begin(leg, other + 2 * count * side)
        recv[leg, me] = send[leg, me]

    def pack(parity, rows_at, pair):
        high, low = split(jnp.concatenate(pair, axis=0))
        at = slice(rows_at[1] * LANES, (rows_at[1] + 1) * LANES)
        first = rows_at[0] * 2 * quarter
        packed[parity, first : first + 2 * quarter, at] = high
        packed[parity, band + first : band + first + 2 * quarter, at] = low

    def turned(leg, g):
        return block_transpose([recv[leg, 4 * g + k] for k in range(4)])

    def dots(parity, high, low):
        dot = functools.partial(jnp.dot, preferred_element_type=jnp.float32)
        both = packed[parity]
        out = dot(both, high)
        return out[:band] + out[band:] + dot(both[:band], low)

    def land_forward(leg):
        all_of(leg).wait_recv()
        groups = devices // 8
        for g in range(groups):
            first, second = turned(leg, g), turned(leg, g + groups)
            for pair in range(2):
                a = [first[2 * pair], first[2 * pair + 1]]
                b = [second[2 * pair], second[2 * pair + 1]]
                pack(0, (pair, g), [m + n for m, n in zip(a, b)])
                pack(1, (pair, g), [m - n for m, n in zip(a, b)])
        return jnp.concatenate(
            [dots(0, forth[0, 0], forth[0, 1]), dots(1, flipped[0], flipped[1])], axis=1
        )

    def land_inverse(leg):
        all_of(leg).wait_recv()
        groups = devices // 8
        for parity in range(2):
            for g in range(groups):
                pieces = turned(leg, parity * groups + g)
                for pair in range(2):
                    pack(parity, (pair, g), [pieces[2 * pair], pieces[2 * pair + 1]])
        first = dots(0, forth[0, 0], forth[0, 1])
        second = dots(1, forth[1, 0], forth[1, 1])
        return first + second, first - second

    def gathered(field, start):
        return jnp.concatenate([x_in[field, start + block] for block in range(cols // 2)], axis=1)

    def spread_field(lower, upper):
        spread(0, lower + upper)
        spread(1, lower - upper)

    def halves(field):
        return gathered(field, 0), gathered(field, cols // 2)

    for copy in in_copies[1]:
        copy.wait_recv()
    spread_field(*halves(1))
    pl.semaphore_wait(ready, rows - 1)
    forward(0)
    for copy in in_copies[0]:
        copy.wait_recv()
    spread_field(*(u * v * v for u, v in zip(halves(0), halves(1))))
    forward(1)
    spread_field(*halves(0))
    forward(2)
    build(flipped, 2, 4)
    fill_filters()

    def spread_spectrum(values):
        spread(0, values[:, :half])
        spread(1, values[:, half:])

    activator = filters[2] * land_forward(0)
    reaction = land_forward(1)
    spread_spectrum(activator + filters[3] * reaction)
    spectrum[...] = filters[1] * reaction
    inverse(3)
    spread_spectrum(filters[0] * land_forward(2) - spectrum[...])
    inverse(4)

    def out_copy(step, field):
        other = lax.rem(col + step, cols)
        return pltpu.make_async_remote_copy(
            src_ref=result.at[field, other],
            dst_ref=sections.at[field, pl.ds(pl.multiple_of(col * band, band), band)],
            send_sem=out_send.at[field, step],
            recv_sem=out_recv.at[field, step],
            device_id=(row, other),
            device_id_type=MESH,
        )

    out_copies = []
    for leg, field in ((3, 1), (4, 0)):
        for side, out in enumerate(land_inverse(leg)):
            for block in range(cols // 2):
                at = slice(block * half * 2 // cols, (block + 1) * half * 2 // cols)
                result[field, side * (cols // 2) + block] = out[:, at]
        for step in range(1, cols):
            out_copies.append(out_copy(step, field))
            out_copies[-1].start()
        sections[field, pl.ds(pl.multiple_of(col * band, band), band)] = result[field, col]
    for copy in in_copies[0] + in_copies[1]:
        copy.wait_send()
    for leg in range(5):
        all_of(leg).wait_send()
    for copy in out_copies:
        copy.wait()


def tables(total, group):
    half = total // 2
    short, wave = np.arange(group), np.arange(half)
    coarse = np.arange(half // group) * group

    def angles(left, right):
        return 2.0 * np.pi / total * (left[:, None] * right[None, :] % total)

    parts = []
    for fine in (
        angles(2 * short, wave), angles(2 * short + 1, wave), angles(short, 2 * wave + 1)
    ):
        parts += [np.cos(fine) + np.sin(fine), np.cos(fine) - np.sin(fine)]
    for rough in (angles(2 * coarse, wave), angles(coarse, 2 * wave + 1)):
        parts += [np.cos(rough), np.sin(rough)]
    parts = [np.pad(part, ((0, group - part.shape[0]), (0, 0))) for part in parts]
    return jnp.asarray(np.stack(parts), jnp.float32)


def on_device_fused(rows, cols, substrate, activator):
    height, width = substrate.shape
    total = width * cols
    band = height // cols
    devices = rows * cols
    half = total // 2
    bf16, f32 = jnp.bfloat16, jnp.float32
    dma = pltpu.SemaphoreType.DMA
    vmem = pl.BlockSpec(memory_space=pltpu.VMEM)
    operands = (substrate, activator, tables(total, 32))
    sections = pl.pallas_call(
        functools.partial(section_kernel, rows, cols),
        out_shape=jax.ShapeDtypeStruct((2,) + substrate.shape, f32),
        in_specs=[pl.BlockSpec(memory_space=pltpu.HBM)] * 3,
        out_specs=vmem,
        scratch_shapes=[
            pltpu.VMEM(substrate.shape, f32),
            pltpu.VMEM(substrate.shape, f32),
            pltpu.VMEM((10, 32, half), f32),
            pltpu.VMEM((2, 2, half, half), bf16),
            pltpu.VMEM((2, half, half), bf16),
            pltpu.VMEM((2, cols, band, width), f32),
            pltpu.VMEM((2, 2 * band, half), bf16),
            pltpu.VMEM((2, 8 * band, half), bf16),
            pltpu.VMEM((4, band, total), f32),
            pltpu.VMEM((band, total), f32),
            pltpu.VMEM((5, devices, band // 4, LANES), f32),
            pltpu.VMEM((5, devices, band // 4, LANES), f32),
            pltpu.VMEM((2, cols, band, width), f32),
            pltpu.SemaphoreType.REGULAR,
            dma((3,)),
            dma((2, cols)),
            dma((2, cols)),
            dma((5,)),
            dma((5,)),
            dma((2, cols)),
            dma((2, cols)),
        ],
        compiler_params=pltpu.CompilerParams(
            collective_id=0, has_side_effects=True, vmem_limit_bytes=48 * 2**20
        ),
    )(*(pltpu.with_memory_space_constraint(value, pltpu.HBM) for value in operands))
    zero = -(FEED_RATE)
    constant = FEED_RATE * math.expm1(zero * 0.5 * TIME_STEP) / zero
    normalize = 1.0 / (total * total)
    return sections[0] * normalize + constant, sections[1] * normalize


def dispatch(rows, cols, substrate, activator):
    height, width = substrate.shape
    total = width * cols
    band = height // cols
    dense_fits = total * total * 4 <= 16 * 2**20
    fits = height * rows == total and 4 * band == LANES and band * rows * cols == total
    if fits and dense_fits and width == 256:
        return on_device_fused(rows, cols, substrate, activator)
    return on_device(substrate, activator)


def solution(mesh):
    in_specs = (P("row", "col"), P("row", "col"))
    out_specs = (P("row", "col"), P("row", "col"))
    return jax.shard_map(
        functools.partial(dispatch, mesh.shape["row"], mesh.shape["col"]),
        mesh=mesh,
        in_specs=in_specs,
        out_specs=out_specs,
        check_vma=False,
    )
```

```python
import functools
import math

import jax
import jax.numpy as jnp
import numpy as np
from jax import lax
from jax.experimental import pallas as pl
from jax.experimental.pallas import tpu as pltpu
from jax.sharding import PartitionSpec as P

FEED_RATE = 0.037
KILL_RATE = 0.06
TIME_STEP = 8.0
SUBSTRATE_DIFFUSION = 4e-07
ACTIVATOR_DIFFUSION = 2e-07


def rotation(left_index, right_index, period, direction):
    phase_index = left_index * right_index % period
    angles = phase_index.astype(jnp.float32) * (2.0 * math.pi / period)
    return (jnp.cos(angles), direction * jnp.sin(angles))


def complex_matrix(size_count, direction):
    indices = jnp.arange(size_count, dtype=jnp.int32)
    cosine_part, sine_part = rotation(indices[:, None], indices[None, :], size_count, direction)
    return jnp.stack([jnp.stack([cosine_part, -sine_part]), jnp.stack([sine_part, cosine_part])])


def transform_last(values, direction):
    part_count, species, middle, length = values.shape
    leading = 64
    second = length // leading
    shaped = values.reshape(part_count, species, middle, leading, second)
    first_matrix = complex_matrix(leading, direction)
    first_pass = jnp.einsum(
        "pqka,qsmab->psmkb", first_matrix, shaped, precision=lax.Precision.HIGHEST
    )
    cosine_part, sine_part = rotation(
        jnp.arange(leading, dtype=jnp.int32)[:, None],
        jnp.arange(second, dtype=jnp.int32)[None, :],
        length,
        direction,
    )
    turned = jnp.stack(
        [
            first_pass[0] * cosine_part - first_pass[1] * sine_part,
            first_pass[0] * sine_part + first_pass[1] * cosine_part,
        ]
    )
    second_matrix = complex_matrix(second, direction)
    second_pass = jnp.einsum(
        "pqkb,qsmjb->psmkj", second_matrix, turned, precision=lax.Precision.HIGHEST
    )
    return second_pass.reshape(part_count, species, middle, length)


def signed_squares(wave_index, total):
    signed = jnp.where(2 * wave_index < total, wave_index, wave_index - total).astype(jnp.float32)
    angular = 2.0 * math.pi * signed
    return angular * angular


def section_factors(row_wave, col_wave, total_rows, total_cols):
    wave_number = signed_squares(row_wave, total_rows) + signed_squares(col_wave, total_cols)
    normalize = 1.0 / (total_rows * total_cols)
    growths = []
    forcings = []
    for diffusion, decay_rate in (
        (SUBSTRATE_DIFFUSION, FEED_RATE),
        (ACTIVATOR_DIFFUSION, FEED_RATE + KILL_RATE),
    ):
        linear = -diffusion * wave_number - decay_rate
        exponent = linear * (0.5 * TIME_STEP)
        growths.append(jnp.exp(exponent) * normalize)
        forcings.append(jnp.expm1(exponent) / linear * normalize)
    return (jnp.stack(growths), jnp.stack(forcings))


def advance(spectra, growth, forcing):
    real_part = spectra[0]
    imag_part = spectra[1]
    return jnp.stack(
        [growth * real_part + forcing * imag_part, growth * imag_part - forcing * real_part]
    )


def col_forward(values):
    return lax.all_to_all(values, "col", split_axis=2, concat_axis=3, tiled=True)


def col_backward(values):
    return lax.all_to_all(values, "col", split_axis=3, concat_axis=2, tiled=True)


def row_forward(values):
    return lax.all_to_all(values, "row", split_axis=2, concat_axis=3, tiled=True)


def row_backward(values):
    return lax.all_to_all(values, "row", split_axis=3, concat_axis=2, tiled=True)


def on_device(substrate, activator):
    row_count, col_count = substrate.shape
    total_rows = row_count * lax.axis_size("row")
    total_cols = col_count * lax.axis_size("col")
    row_index = lax.axis_index("row")
    col_index = lax.axis_index("col")
    reaction = substrate * activator * activator
    fields = jnp.stack(
        [jnp.stack([substrate, activator]), jnp.stack([FEED_RATE - reaction, reaction])]
    )
    spectra = transform_last(col_forward(fields), -1)
    spectra = row_forward(col_forward(jnp.swapaxes(spectra, 2, 3)))
    spectra = transform_last(spectra, -1)
    local_cols = col_count // lax.axis_size("row")
    col_wave = (
        col_count * col_index
        + local_cols * row_index
        + jnp.arange(local_cols, dtype=jnp.int32)[:, None]
    )
    row_wave = jnp.arange(total_rows, dtype=jnp.int32)[None, :]
    growth, forcing = section_factors(row_wave, col_wave, total_rows, total_cols)
    spectra = transform_last(advance(spectra, growth, forcing), 1)
    spectra = col_backward(row_backward(spectra))
    spectra = jnp.swapaxes(spectra, 2, 3)
    spectra = transform_last(spectra, 1)
    fields = lax.all_to_all(spectra[:1], "col", split_axis=3, concat_axis=2, tiled=True)
    return (fields[0, 0], fields[0, 1])


MESH = pl.DeviceIdType.MESH
LANES = 128


def split(values):
    high = values.astype(jnp.bfloat16)
    low = (values - high.astype(jnp.float32)).astype(jnp.bfloat16)
    return high, low


def contract_last(left, right):
    return lax.dot_general(
        left, right, (((1,), (1,)), ((), ())), preferred_element_type=jnp.float32
    )


def block_transpose(pieces):
    first, second, third, fourth = pieces
    lane = lax.broadcasted_iota(jnp.int32, first.shape, 1)
    upper = lane < LANES // 2
    even = lane // (LANES // 4) % 2 == 0

    def far(a, b):
        return (
            jnp.where(upper, a, pltpu.roll(b, LANES // 2, 1)),
            jnp.where(upper, pltpu.roll(a, LANES // 2, 1), b),
        )

    def near(a, b):
        return (
            jnp.where(even, a, pltpu.roll(b, LANES // 4, 1)),
            jnp.where(even, pltpu.roll(a, 3 * LANES // 4, 1), b),
        )

    first, third = far(first, third)
    second, fourth = far(second, fourth)
    first, second = near(first, second)
    third, fourth = near(third, fourth)
    return first, second, third, fourth


def section_kernel(
    rows, cols, u_hbm, v_hbm, tables_hbm, sections, u_ref, v_ref, tables_ref,
    forth, flipped, x_in, packed, wide, filters, spectrum, send, recv, result,
    ready, load_sem, in_send, in_recv, s_send, s_recv, out_send, out_recv,
):
    devices = rows * cols
    total = u_ref.shape[1] * cols
    half = total // 2
    band = u_ref.shape[0] // cols
    quarter = band // 4
    chunk = half // 2
    group = 32
    row = lax.axis_index("row")
    col = lax.axis_index("col")
    me = row * cols + col

    loads = [
        pltpu.make_async_copy(source, target, load_sem.at[index])
        for index, (source, target) in enumerate(
            ((v_hbm, v_ref), (u_hbm, u_ref), (tables_hbm, tables_ref))
        )
    ]
    for load in loads:
        load.start()
    barrier = pltpu.get_barrier_semaphore()

    def greet(semaphore, other_row, other_col):
        pl.semaphore_signal(
            semaphore, inc=1, device_id=(other_row, other_col), device_id_type=MESH
        )

    for step in range(1, cols):
        greet(barrier, row, lax.rem(col + step, cols))
    for step in range(1, rows):
        greet(barrier, lax.rem(row + step, rows), col)
    for load in loads[:2]:
        load.wait()
    pl.semaphore_wait(barrier, rows + cols - 2)

    def in_copy(step, field):
        ref = (u_ref, v_ref)[field]
        other = lax.rem(col + step, cols)
        return pltpu.make_async_remote_copy(
            src_ref=ref.at[pl.ds(pl.multiple_of(other * band, band), band)],
            dst_ref=x_in.at[field, col],
            send_sem=in_send.at[0],
            recv_sem=in_recv.at[field],
            device_id=(row, other),
            device_id_type=MESH,
        )

    for field in (1, 0):
        for step in range(1, cols):
            in_copy(step, field).start()
    for step in range(1, rows):
        greet(ready, lax.rem(row + step, rows), col)
    for field, ref in enumerate((u_ref, v_ref)):
        x_in[field, col] = ref[pl.ds(pl.multiple_of(col * band, band), band)]
    loads[2].wait()

    def build(target, coarse, fine):
        def body(step, carry):
            cosine = tables_ref[6 + coarse, pl.ds(step, 1)]
            sine = tables_ref[7 + coarse, pl.ds(step, 1)]
            high, low = split(cosine * tables_ref[fine] + sine * tables_ref[fine + 1])
            at = pl.ds(pl.multiple_of(step * group, group), group)
            target[0, at] = high
            target[1, at] = low
            return carry

        lax.fori_loop(0, half // group, body, 0)

    build(forth.at[0], 0, 0)
    build(forth.at[1], 0, 2)

    def wave(position):
        return jnp.where(position < half, 2 * position, 2 * (position - half) + 1)

    def fill_filters():
        shape = (band, total)
        q = wave(me * band + lax.broadcasted_iota(jnp.int32, shape, 0))
        p = wave(lax.broadcasted_iota(jnp.int32, shape, 1))
        wave_number = signed_squares(p, total) + signed_squares(q, total)
        for index, (diffusion, decay_rate) in enumerate((
            (SUBSTRATE_DIFFUSION, FEED_RATE),
            (ACTIVATOR_DIFFUSION, FEED_RATE + KILL_RATE),
        )):
            linear = -diffusion * wave_number - decay_rate
            growth = jnp.exp(linear * (0.5 * TIME_STEP))
            filters[2 * index] = growth
            filters[2 * index + 1] = (growth - 1.0) / linear

    def remote(leg, other):
        return pltpu.make_async_remote_copy(
            src_ref=send.at[leg, other],
            dst_ref=recv.at[leg, me],
            send_sem=s_send.at[0],
            recv_sem=s_recv.at[leg],
            device_id=(other // cols, lax.rem(other, cols)),
            device_id_type=MESH,
        )

    def all_of(source, target, send_sem, recv_sem):
        return pltpu.make_async_remote_copy(
            src_ref=source,
            dst_ref=target,
            send_sem=send_sem,
            recv_sem=recv_sem,
            device_id=(row, lax.rem(col + 1, cols)),
            device_id_type=MESH,
        )

    def arrived(leg):
        blocks = recv.at[leg, pl.ds(0, devices - 1)]
        all_of(blocks, blocks, s_send.at[0], s_recv.at[leg]).wait_recv()

    def gather(field):
        blocks = x_in.at[field, pl.ds(0, cols - 1)]
        all_of(blocks, blocks, in_send.at[0], in_recv.at[field]).wait_recv()

    def spread(parity, field):
        high, low = split(field)
        for copy_at in range(4):
            wide[parity, copy_at * band : (copy_at + 1) * band] = high
            wide[parity, (4 + copy_at) * band : (5 + copy_at) * band] = low

    def product(high, low, parity):
        both = contract_last(high, wide[parity])
        return both[:, :LANES] + both[:, LANES:] + contract_last(low, wide[parity, :LANES])

    def stage(leg, first, values):
        count = values.shape[0] // band
        lane = lax.broadcasted_iota(jnp.int32, (count, quarter, LANES), 2) // (LANES // 4)
        out = values.reshape(count, band, LANES)
        piece = out[:, :quarter]
        for j in range(1, 4):
            piece = jnp.where(lane == j, out[:, j * quarter : (j + 1) * quarter], piece)
        send[leg, pl.ds(first, count)] = piece


    def begin(leg):
        for step in range(1, devices):
            over = step - 1 if step < cols else step
            turn = (3, 1, 2, 0)[over % cols]
            other_row = lax.rem(row + over // cols, rows)
            remote(leg, other_row * cols + lax.rem(col + turn, cols)).start()
        recv[leg, me] = send[leg, me]

    def forward(leg):
        for parity in range(2):
            stage(
                leg,
                parity * (devices // 2),
                product(forth[parity, 0], forth[parity, 1], parity),
            )
        begin(leg)

    def inverse(leg):
        count = devices // 4
        for part in range(2):
            at = slice(part * chunk, (part + 1) * chunk)
            first = product(forth[0, 0, at], forth[0, 1, at], 0)
            second = product(flipped[0, at], flipped[1, at], 1)
            stage(leg, part * count, first + second)
            stage(leg, part * count + 2 * count, first - second)
        begin(leg)

    def pack(parity, rows_at, pair):
        high, low = split(jnp.concatenate(pair, axis=0))
        at = slice(rows_at[1] * LANES, (rows_at[1] + 1) * LANES)
        first = rows_at[0] * 2 * quarter
        packed[parity, first : first + 2 * quarter, at] = high
        packed[parity, band + first : band + first + 2 * quarter, at] = low

    def turned(leg, g):
        return block_transpose([recv[leg, 4 * g + k] for k in range(4)])

    def dots(parity, high, low):
        dot = functools.partial(jnp.dot, preferred_element_type=jnp.float32)
        both = packed[parity]
        out = dot(both, high)
        return out[:band] + out[band:] + dot(both[:band], low)

    def land_forward(leg):
        arrived(leg)
        groups = devices // 8
        for g in range(groups):
            first, second = turned(leg, g), turned(leg, g + groups)
            for pair in range(2):
                a = [first[2 * pair], first[2 * pair + 1]]
                b = [second[2 * pair], second[2 * pair + 1]]
                pack(0, (pair, g), [m + n for m, n in zip(a, b)])
                pack(1, (pair, g), [m - n for m, n in zip(a, b)])
        return jnp.concatenate(
            [dots(0, forth[0, 0], forth[0, 1]), dots(1, flipped[0], flipped[1])], axis=1
        )

    def land_inverse(leg):
        arrived(leg)
        groups = devices // 8
        for parity in range(2):
            for g in range(groups):
                pieces = turned(leg, parity * groups + g)
                for pair in range(2):
                    pack(parity, (pair, g), [pieces[2 * pair], pieces[2 * pair + 1]])
        first = dots(0, forth[0, 0], forth[0, 1])
        second = dots(1, forth[1, 0], forth[1, 1])
        return first + second, first - second

    def gathered(field, start):
        return jnp.concatenate([x_in[field, start + block] for block in range(cols // 2)], axis=1)

    def spread_field(lower, upper):
        spread(0, lower + upper)
        spread(1, lower - upper)

    def halves(field):
        return gathered(field, 0), gathered(field, cols // 2)

    gather(1)
    spread_field(*halves(1))
    pl.semaphore_wait(ready, rows - 1)
    forward(0)
    gather(0)
    spread_field(*(u * v * v for u, v in zip(halves(0), halves(1))))
    forward(1)
    spread_field(*halves(0))
    forward(2)
    build(flipped, 2, 4)
    fill_filters()

    def spread_spectrum(values):
        spread(0, values[:, :half])
        spread(1, values[:, half:])

    activator = filters[2] * land_forward(0)
    reaction = land_forward(1)
    spread_spectrum(activator + filters[3] * reaction)
    spectrum[...] = filters[1] * reaction
    inverse(3)
    spread_spectrum(filters[0] * land_forward(2) - spectrum[...])
    inverse(4)

    def out_copy(step, field):
        other = lax.rem(col + step, cols)
        return pltpu.make_async_remote_copy(
            src_ref=result.at[field, other],
            dst_ref=sections.at[field, pl.ds(pl.multiple_of(col * band, band), band)],
            send_sem=out_send.at[0],
            recv_sem=out_recv.at[0],
            device_id=(row, other),
            device_id_type=MESH,
        )

    for leg, field in ((3, 1), (4, 0)):
        for side, out in enumerate(land_inverse(leg)):
            for block in range(cols // 2):
                at = slice(block * half * 2 // cols, (block + 1) * half * 2 // cols)
                result[field, side * (cols // 2) + block] = out[:, at]
        for step in range(1, cols):
            out_copy(step, field).start()
        sections[field, pl.ds(pl.multiple_of(col * band, band), band)] = result[field, col]
    sent = send.at[:, pl.ds(0, devices - 1)]
    all_of(sent, sent, s_send.at[0], s_recv.at[0]).wait_send()
    sent = x_in.at[:, pl.ds(0, cols - 1)]
    all_of(sent, sent, in_send.at[0], in_recv.at[0]).wait_send()
    sent = result.at[:, pl.ds(0, cols - 1)]
    all_of(sent, sent, out_send.at[0], out_recv.at[0]).wait()


def tables(total, group):
    half = total // 2
    short, wave = np.arange(group), np.arange(half)
    coarse = np.arange(half // group) * group

    def angles(left, right):
        return 2.0 * np.pi / total * (left[:, None] * right[None, :] % total)

    parts = []
    for fine in (
        angles(2 * short, wave), angles(2 * short + 1, wave), angles(short, 2 * wave + 1)
    ):
        parts += [np.cos(fine) + np.sin(fine), np.cos(fine) - np.sin(fine)]
    for rough in (angles(2 * coarse, wave), angles(coarse, 2 * wave + 1)):
        parts += [np.cos(rough), np.sin(rough)]
    parts = [np.pad(part, ((0, group - part.shape[0]), (0, 0))) for part in parts]
    return jnp.asarray(np.stack(parts), jnp.float32)


def on_device_fused(rows, cols, substrate, activator):
    height, width = substrate.shape
    total = width * cols
    band = height // cols
    devices = rows * cols
    half = total // 2
    bf16, f32 = jnp.bfloat16, jnp.float32
    dma = pltpu.SemaphoreType.DMA
    vmem = pl.BlockSpec(memory_space=pltpu.VMEM)
    operands = (substrate, activator, tables(total, 32))
    sections = pl.pallas_call(
        functools.partial(section_kernel, rows, cols),
        out_shape=jax.ShapeDtypeStruct((2,) + substrate.shape, f32),
        in_specs=[pl.BlockSpec(memory_space=pltpu.HBM)] * 3,
        out_specs=vmem,
        scratch_shapes=[
            pltpu.VMEM(substrate.shape, f32),
            pltpu.VMEM(substrate.shape, f32),
            pltpu.VMEM((10, 32, half), f32),
            pltpu.VMEM((2, 2, half, half), bf16),
            pltpu.VMEM((2, half, half), bf16),
            pltpu.VMEM((2, cols, band, width), f32),
            pltpu.VMEM((2, 2 * band, half), bf16),
            pltpu.VMEM((2, 8 * band, half), bf16),
            pltpu.VMEM((4, band, total), f32),
            pltpu.VMEM((band, total), f32),
            pltpu.VMEM((5, devices, band // 4, LANES), f32),
            pltpu.VMEM((5, devices, band // 4, LANES), f32),
            pltpu.VMEM((2, cols, band, width), f32),
            pltpu.SemaphoreType.REGULAR,
            dma((3,)),
            dma((1,)),
            dma((2,)),
            dma((1,)),
            dma((5,)),
            dma((1,)),
            dma((1,)),
        ],
        compiler_params=pltpu.CompilerParams(
            collective_id=0, has_side_effects=True, vmem_limit_bytes=48 * 2**20
        ),
    )(*(pltpu.with_memory_space_constraint(value, pltpu.HBM) for value in operands))
    zero = -(FEED_RATE)
    constant = FEED_RATE * math.expm1(zero * 0.5 * TIME_STEP) / zero
    normalize = 1.0 / (total * total)
    return sections[0] * normalize + constant, sections[1] * normalize


def dispatch(rows, cols, substrate, activator):
    height, width = substrate.shape
    total = width * cols
    band = height // cols
    dense_fits = total * total * 4 <= 16 * 2**20
    fits = height * rows == total and 4 * band == LANES and band * rows * cols == total
    if fits and dense_fits and width == 256:
        return on_device_fused(rows, cols, substrate, activator)
    return on_device(substrate, activator)


def solution(mesh):
    in_specs = (P("row", "col"), P("row", "col"))
    out_specs = (P("row", "col"), P("row", "col"))
    return jax.shard_map(
        functools.partial(dispatch, mesh.shape["row"], mesh.shape["col"]),
        mesh=mesh,
        in_specs=in_specs,
        out_specs=out_specs,
        check_vma=False,
    )
```

```python
import functools
import math

import jax
import jax.numpy as jnp
import numpy as np
from jax import lax
from jax.experimental import pallas as pl
from jax.experimental.pallas import tpu as pltpu
from jax.sharding import PartitionSpec as P

FEED_RATE = 0.037
KILL_RATE = 0.06
TIME_STEP = 8.0
SUBSTRATE_DIFFUSION = 4e-07
ACTIVATOR_DIFFUSION = 2e-07


def rotation(left_index, right_index, period, direction):
    phase_index = left_index * right_index % period
    angles = phase_index.astype(jnp.float32) * (2.0 * math.pi / period)
    return (jnp.cos(angles), direction * jnp.sin(angles))


def complex_matrix(size_count, direction):
    indices = jnp.arange(size_count, dtype=jnp.int32)
    cosine_part, sine_part = rotation(indices[:, None], indices[None, :], size_count, direction)
    return jnp.stack([jnp.stack([cosine_part, -sine_part]), jnp.stack([sine_part, cosine_part])])


def transform_last(values, direction):
    part_count, species, middle, length = values.shape
    leading = 64
    second = length // leading
    shaped = values.reshape(part_count, species, middle, leading, second)
    first_matrix = complex_matrix(leading, direction)
    first_pass = jnp.einsum(
        "pqka,qsmab->psmkb", first_matrix, shaped, precision=lax.Precision.HIGHEST
    )
    cosine_part, sine_part = rotation(
        jnp.arange(leading, dtype=jnp.int32)[:, None],
        jnp.arange(second, dtype=jnp.int32)[None, :],
        length,
        direction,
    )
    turned = jnp.stack(
        [
            first_pass[0] * cosine_part - first_pass[1] * sine_part,
            first_pass[0] * sine_part + first_pass[1] * cosine_part,
        ]
    )
    second_matrix = complex_matrix(second, direction)
    second_pass = jnp.einsum(
        "pqkb,qsmjb->psmkj", second_matrix, turned, precision=lax.Precision.HIGHEST
    )
    return second_pass.reshape(part_count, species, middle, length)


def signed_squares(wave_index, total):
    signed = jnp.where(2 * wave_index < total, wave_index, wave_index - total).astype(jnp.float32)
    angular = 2.0 * math.pi * signed
    return angular * angular


def section_factors(row_wave, col_wave, total_rows, total_cols):
    wave_number = signed_squares(row_wave, total_rows) + signed_squares(col_wave, total_cols)
    normalize = 1.0 / (total_rows * total_cols)
    growths = []
    forcings = []
    for diffusion, decay_rate in (
        (SUBSTRATE_DIFFUSION, FEED_RATE),
        (ACTIVATOR_DIFFUSION, FEED_RATE + KILL_RATE),
    ):
        linear = -diffusion * wave_number - decay_rate
        exponent = linear * (0.5 * TIME_STEP)
        growths.append(jnp.exp(exponent) * normalize)
        forcings.append(jnp.expm1(exponent) / linear * normalize)
    return (jnp.stack(growths), jnp.stack(forcings))


def advance(spectra, growth, forcing):
    real_part = spectra[0]
    imag_part = spectra[1]
    return jnp.stack(
        [growth * real_part + forcing * imag_part, growth * imag_part - forcing * real_part]
    )


def col_forward(values):
    return lax.all_to_all(values, "col", split_axis=2, concat_axis=3, tiled=True)


def col_backward(values):
    return lax.all_to_all(values, "col", split_axis=3, concat_axis=2, tiled=True)


def row_forward(values):
    return lax.all_to_all(values, "row", split_axis=2, concat_axis=3, tiled=True)


def row_backward(values):
    return lax.all_to_all(values, "row", split_axis=3, concat_axis=2, tiled=True)


def on_device(substrate, activator):
    row_count, col_count = substrate.shape
    total_rows = row_count * lax.axis_size("row")
    total_cols = col_count * lax.axis_size("col")
    row_index = lax.axis_index("row")
    col_index = lax.axis_index("col")
    reaction = substrate * activator * activator
    fields = jnp.stack(
        [jnp.stack([substrate, activator]), jnp.stack([FEED_RATE - reaction, reaction])]
    )
    spectra = transform_last(col_forward(fields), -1)
    spectra = row_forward(col_forward(jnp.swapaxes(spectra, 2, 3)))
    spectra = transform_last(spectra, -1)
    local_cols = col_count // lax.axis_size("row")
    col_wave = (
        col_count * col_index
        + local_cols * row_index
        + jnp.arange(local_cols, dtype=jnp.int32)[:, None]
    )
    row_wave = jnp.arange(total_rows, dtype=jnp.int32)[None, :]
    growth, forcing = section_factors(row_wave, col_wave, total_rows, total_cols)
    spectra = transform_last(advance(spectra, growth, forcing), 1)
    spectra = col_backward(row_backward(spectra))
    spectra = jnp.swapaxes(spectra, 2, 3)
    spectra = transform_last(spectra, 1)
    fields = lax.all_to_all(spectra[:1], "col", split_axis=3, concat_axis=2, tiled=True)
    return (fields[0, 0], fields[0, 1])


MESH = pl.DeviceIdType.MESH
LANES = 128


def split(values):
    high = values.astype(jnp.bfloat16)
    low = (values - high.astype(jnp.float32)).astype(jnp.bfloat16)
    return high, low


def contract_last(left, right):
    return lax.dot_general(
        left, right, (((1,), (1,)), ((), ())), preferred_element_type=jnp.float32
    )


def block_transpose(pieces):
    first, second, third, fourth = pieces
    lane = lax.broadcasted_iota(jnp.int32, first.shape, 1)
    upper = lane < LANES // 2
    even = lane // (LANES // 4) % 2 == 0

    def far(a, b):
        return (
            jnp.where(upper, a, pltpu.roll(b, LANES // 2, 1)),
            jnp.where(upper, pltpu.roll(a, LANES // 2, 1), b),
        )

    def near(a, b):
        return (
            jnp.where(even, a, pltpu.roll(b, LANES // 4, 1)),
            jnp.where(even, pltpu.roll(a, 3 * LANES // 4, 1), b),
        )

    first, third = far(first, third)
    second, fourth = far(second, fourth)
    first, second = near(first, second)
    third, fourth = near(third, fourth)
    return first, second, third, fourth


def section_kernel(
    rows, cols, u_hbm, v_hbm, tables_hbm, sections, u_ref, v_ref, tables_ref,
    forth, flipped, x_in, packed, wide, filters, spectrum, send, recv, result,
    ready, load_sem, in_send, in_recv, s_send, s_recv, out_send, out_recv,
):
    devices = rows * cols
    total = u_ref.shape[1] * cols
    half = total // 2
    band = u_ref.shape[0] // cols
    quarter = band // 4
    chunk = half // 2
    group = 32
    row = lax.axis_index("row")
    col = lax.axis_index("col")
    me = row * cols + col

    loads = [
        pltpu.make_async_copy(source, target, load_sem.at[index])
        for index, (source, target) in enumerate(
            ((v_hbm, v_ref), (u_hbm, u_ref), (tables_hbm, tables_ref))
        )
    ]
    for load in loads:
        load.start()
    barrier = pltpu.get_barrier_semaphore()

    def greet(semaphore, other_row, other_col):
        pl.semaphore_signal(
            semaphore, inc=1, device_id=(other_row, other_col), device_id_type=MESH
        )

    for step in range(1, cols):
        greet(barrier, row, lax.rem(col + step, cols))
    for step in range(1, rows):
        greet(barrier, lax.rem(row + step, rows), col)
    pl.semaphore_wait(barrier, rows + cols - 2)

    def in_copy(step, field):
        ref = (u_ref, v_ref)[field]
        other = lax.rem(col + step, cols)
        return pltpu.make_async_remote_copy(
            src_ref=ref.at[pl.ds(pl.multiple_of(other * band, band), band)],
            dst_ref=x_in.at[field, col],
            send_sem=in_send.at[0],
            recv_sem=in_recv.at[field],
            device_id=(row, other),
            device_id_type=MESH,
        )

    for field in (1, 0):
        loads[1 - field].wait()
        for step in range(1, cols):
            in_copy(step, field).start()
    for step in range(1, rows):
        greet(ready, lax.rem(row + step, rows), col)
    for field, ref in enumerate((u_ref, v_ref)):
        x_in[field, col] = ref[pl.ds(pl.multiple_of(col * band, band), band)]
    loads[2].wait()

    def build(target, coarse, fine):
        def body(step, carry):
            cosine = tables_ref[6 + coarse, pl.ds(step, 1)]
            sine = tables_ref[7 + coarse, pl.ds(step, 1)]
            high, low = split(cosine * tables_ref[fine] + sine * tables_ref[fine + 1])
            at = pl.ds(pl.multiple_of(step * group, group), group)
            target[0, at] = high
            target[1, at] = low
            return carry

        lax.fori_loop(0, half // group, body, 0)

    build(forth.at[0], 0, 0)
    build(forth.at[1], 0, 2)

    def wave(position):
        return jnp.where(position < half, 2 * position, 2 * (position - half) + 1)

    def fill_filters():
        shape = (band, total)
        q = wave(me * band + lax.broadcasted_iota(jnp.int32, shape, 0))
        p = wave(lax.broadcasted_iota(jnp.int32, shape, 1))
        wave_number = signed_squares(p, total) + signed_squares(q, total)
        for index, (diffusion, decay_rate) in enumerate((
            (SUBSTRATE_DIFFUSION, FEED_RATE),
            (ACTIVATOR_DIFFUSION, FEED_RATE + KILL_RATE),
        )):
            linear = -diffusion * wave_number - decay_rate
            growth = jnp.exp(linear * (0.5 * TIME_STEP))
            filters[2 * index] = growth
            filters[2 * index + 1] = (growth - 1.0) / linear

    def remote(leg, other):
        return pltpu.make_async_remote_copy(
            src_ref=send.at[leg, other],
            dst_ref=recv.at[leg, me],
            send_sem=s_send.at[0],
            recv_sem=s_recv.at[leg],
            device_id=(other // cols, lax.rem(other, cols)),
            device_id_type=MESH,
        )

    def all_of(source, target, send_sem, recv_sem):
        return pltpu.make_async_remote_copy(
            src_ref=source,
            dst_ref=target,
            send_sem=send_sem,
            recv_sem=recv_sem,
            device_id=(row, lax.rem(col + 1, cols)),
            device_id_type=MESH,
        )

    def arrived(leg):
        blocks = recv.at[leg, pl.ds(0, devices - 1)]
        all_of(blocks, blocks, s_send.at[0], s_recv.at[leg]).wait_recv()

    def gather(field):
        blocks = x_in.at[field, pl.ds(0, cols - 1)]
        all_of(blocks, blocks, in_send.at[0], in_recv.at[field]).wait_recv()

    def spread(parity, field):
        high, low = split(field)
        for copy_at in range(4):
            wide[parity, copy_at * band : (copy_at + 1) * band] = high
            wide[parity, (4 + copy_at) * band : (5 + copy_at) * band] = low

    def product(high, low, parity):
        both = contract_last(high, wide[parity])
        return both[:, :LANES] + both[:, LANES:] + contract_last(low, wide[parity, :LANES])

    def stage(leg, first, values):
        count = values.shape[0] // band
        lane = lax.broadcasted_iota(jnp.int32, (count, quarter, LANES), 2) // (LANES // 4)
        out = values.reshape(count, band, LANES)
        piece = out[:, :quarter]
        for j in range(1, 4):
            piece = jnp.where(lane == j, out[:, j * quarter : (j + 1) * quarter], piece)
        send[leg, pl.ds(first, count)] = piece


    def begin(leg):
        for step in range(1, devices):
            over = step - 1 if step < cols else step
            turn = (3, 1, 2, 0)[over % cols]
            other_row = lax.rem(row + over // cols, rows)
            remote(leg, other_row * cols + lax.rem(col + turn, cols)).start()
        recv[leg, me] = send[leg, me]

    def lead(leg):
        count = devices // 2
        for step in range(2):
            parity = lax.rem(me // count + 1 + step, 2)
            stage(leg, parity * count, product(forth[parity, 0], forth[parity, 1], parity))
            for k in range(step, count):
                remote(leg, parity * count + lax.rem(me + k, count)).start()
        recv[leg, me] = send[leg, me]

    def forward(leg):
        for parity in range(2):
            stage(
                leg,
                parity * (devices // 2),
                product(forth[parity, 0], forth[parity, 1], parity),
            )
        begin(leg)

    def swift(leg):
        count = devices // 4
        side = me // (2 * count)
        mine = lax.rem(me, 2 * count) // count
        for step in range(2):
            part = lax.rem(mine + 1 + step, 2)
            at = pl.ds(pl.multiple_of(part * chunk, chunk), chunk)
            first = product(forth[0, 0, at], forth[0, 1, at], 0)
            second = product(flipped[0, at], flipped[1, at], 1)
            stage(leg, part * count, first + second)
            stage(leg, part * count + 2 * count, first - second)
            for away, nearest in ((1 - side, 0), (side, step)):
                for k in range(nearest, count):
                    other = part * count + lax.rem(me + k, count)
                    remote(leg, other + 2 * count * away).start()
        recv[leg, me] = send[leg, me]

    def inverse(leg):
        count = devices // 4
        for part in range(2):
            at = slice(part * chunk, (part + 1) * chunk)
            first = product(forth[0, 0, at], forth[0, 1, at], 0)
            second = product(flipped[0, at], flipped[1, at], 1)
            stage(leg, part * count, first + second)
            stage(leg, part * count + 2 * count, first - second)
        begin(leg)

    def pack(parity, rows_at, pair):
        high, low = split(jnp.concatenate(pair, axis=0))
        at = slice(rows_at[1] * LANES, (rows_at[1] + 1) * LANES)
        first = rows_at[0] * 2 * quarter
        packed[parity, first : first + 2 * quarter, at] = high
        packed[parity, band + first : band + first + 2 * quarter, at] = low

    def turned(leg, g):
        return block_transpose([recv[leg, 4 * g + k] for k in range(4)])

    def dots(parity, high, low):
        dot = functools.partial(jnp.dot, preferred_element_type=jnp.float32)
        both = packed[parity]
        out = dot(both, high)
        return out[:band] + out[band:] + dot(both[:band], low)

    def land_forward(leg):
        arrived(leg)
        groups = devices // 8
        for g in range(groups):
            first, second = turned(leg, g), turned(leg, g + groups)
            for pair in range(2):
                a = [first[2 * pair], first[2 * pair + 1]]
                b = [second[2 * pair], second[2 * pair + 1]]
                pack(0, (pair, g), [m + n for m, n in zip(a, b)])
                pack(1, (pair, g), [m - n for m, n in zip(a, b)])
        return jnp.concatenate(
            [dots(0, forth[0, 0], forth[0, 1]), dots(1, flipped[0], flipped[1])], axis=1
        )

    def land_inverse(leg):
        arrived(leg)
        groups = devices // 8
        for parity in range(2):
            for g in range(groups):
                pieces = turned(leg, parity * groups + g)
                for pair in range(2):
                    pack(parity, (pair, g), [pieces[2 * pair], pieces[2 * pair + 1]])
        first = dots(0, forth[0, 0], forth[0, 1])
        second = dots(1, forth[1, 0], forth[1, 1])
        return first + second, first - second

    def gathered(field, start):
        return jnp.concatenate([x_in[field, start + block] for block in range(cols // 2)], axis=1)

    def spread_field(lower, upper):
        spread(0, lower + upper)
        spread(1, lower - upper)

    def halves(field):
        return gathered(field, 0), gathered(field, cols // 2)

    gather(1)
    spread_field(*halves(1))
    pl.semaphore_wait(ready, rows - 1)
    lead(0)
    gather(0)
    spread_field(*(u * v * v for u, v in zip(halves(0), halves(1))))
    forward(1)
    spread_field(*halves(0))
    forward(2)
    build(flipped, 2, 4)
    fill_filters()

    def spread_spectrum(values):
        spread(0, values[:, :half])
        spread(1, values[:, half:])

    activator = filters[2] * land_forward(0)
    reaction = land_forward(1)
    spread_spectrum(activator + filters[3] * reaction)
    spectrum[...] = filters[1] * reaction
    swift(3)
    spread_spectrum(filters[0] * land_forward(2) - spectrum[...])
    inverse(4)

    def out_copy(step, field):
        other = lax.rem(col + step, cols)
        return pltpu.make_async_remote_copy(
            src_ref=result.at[field, other],
            dst_ref=sections.at[field, pl.ds(pl.multiple_of(col * band, band), band)],
            send_sem=out_send.at[0],
            recv_sem=out_recv.at[0],
            device_id=(row, other),
            device_id_type=MESH,
        )

    for leg, field in ((3, 1), (4, 0)):
        for side, out in enumerate(land_inverse(leg)):
            for block in range(cols // 2):
                at = slice(block * half * 2 // cols, (block + 1) * half * 2 // cols)
                result[field, side * (cols // 2) + block] = out[:, at]
        for step in range(1, cols):
            out_copy(step, field).start()
        sections[field, pl.ds(pl.multiple_of(col * band, band), band)] = result[field, col]
    sent = send.at[:, pl.ds(0, devices - 1)]
    all_of(sent, sent, s_send.at[0], s_recv.at[0]).wait_send()
    sent = x_in.at[:, pl.ds(0, cols - 1)]
    all_of(sent, sent, in_send.at[0], in_recv.at[0]).wait_send()
    sent = result.at[:, pl.ds(0, cols - 1)]
    all_of(sent, sent, out_send.at[0], out_recv.at[0]).wait()


def tables(total, group):
    half = total // 2
    short, wave = np.arange(group), np.arange(half)
    coarse = np.arange(half // group) * group

    def angles(left, right):
        return 2.0 * np.pi / total * (left[:, None] * right[None, :] % total)

    parts = []
    for fine in (
        angles(2 * short, wave), angles(2 * short + 1, wave), angles(short, 2 * wave + 1)
    ):
        parts += [np.cos(fine) + np.sin(fine), np.cos(fine) - np.sin(fine)]
    for rough in (angles(2 * coarse, wave), angles(coarse, 2 * wave + 1)):
        parts += [np.cos(rough), np.sin(rough)]
    parts = [np.pad(part, ((0, group - part.shape[0]), (0, 0))) for part in parts]
    return jnp.asarray(np.stack(parts), jnp.float32)


def on_device_fused(rows, cols, substrate, activator):
    height, width = substrate.shape
    total = width * cols
    band = height // cols
    devices = rows * cols
    half = total // 2
    bf16, f32 = jnp.bfloat16, jnp.float32
    dma = pltpu.SemaphoreType.DMA
    vmem = pl.BlockSpec(memory_space=pltpu.VMEM)
    operands = (substrate, activator, tables(total, 32))
    sections = pl.pallas_call(
        functools.partial(section_kernel, rows, cols),
        out_shape=jax.ShapeDtypeStruct((2,) + substrate.shape, f32),
        in_specs=[pl.BlockSpec(memory_space=pltpu.HBM)] * 3,
        out_specs=vmem,
        scratch_shapes=[
            pltpu.VMEM(substrate.shape, f32),
            pltpu.VMEM(substrate.shape, f32),
            pltpu.VMEM((10, 32, half), f32),
            pltpu.VMEM((2, 2, half, half), bf16),
            pltpu.VMEM((2, half, half), bf16),
            pltpu.VMEM((2, cols, band, width), f32),
            pltpu.VMEM((2, 2 * band, half), bf16),
            pltpu.VMEM((2, 8 * band, half), bf16),
            pltpu.VMEM((4, band, total), f32),
            pltpu.VMEM((band, total), f32),
            pltpu.VMEM((5, devices, band // 4, LANES), f32),
            pltpu.VMEM((5, devices, band // 4, LANES), f32),
            pltpu.VMEM((2, cols, band, width), f32),
            pltpu.SemaphoreType.REGULAR,
            dma((3,)),
            dma((1,)),
            dma((2,)),
            dma((1,)),
            dma((5,)),
            dma((1,)),
            dma((1,)),
        ],
        compiler_params=pltpu.CompilerParams(
            collective_id=0, has_side_effects=True, vmem_limit_bytes=48 * 2**20
        ),
    )(*(pltpu.with_memory_space_constraint(value, pltpu.HBM) for value in operands))
    zero = -(FEED_RATE)
    constant = FEED_RATE * math.expm1(zero * 0.5 * TIME_STEP) / zero
    normalize = 1.0 / (total * total)
    return sections[0] * normalize + constant, sections[1] * normalize


def dispatch(rows, cols, substrate, activator):
    height, width = substrate.shape
    total = width * cols
    band = height // cols
    dense_fits = total * total * 4 <= 16 * 2**20
    fits = height * rows == total and 4 * band == LANES and band * rows * cols == total
    if fits and dense_fits and width == 256:
        return on_device_fused(rows, cols, substrate, activator)
    return on_device(substrate, activator)


def solution(mesh):
    in_specs = (P("row", "col"), P("row", "col"))
    out_specs = (P("row", "col"), P("row", "col"))
    return jax.shard_map(
        functools.partial(dispatch, mesh.shape["row"], mesh.shape["col"]),
        mesh=mesh,
        in_specs=in_specs,
        out_specs=out_specs,
        check_vma=False,
    )
```

```python
import functools
import math

import jax
import jax.numpy as jnp
import numpy as np
from jax import lax
from jax.experimental import pallas as pl
from jax.experimental.pallas import tpu as pltpu
from jax.sharding import PartitionSpec as P

FEED_RATE = 0.037
KILL_RATE = 0.06
TIME_STEP = 8.0
SUBSTRATE_DIFFUSION = 4e-07
ACTIVATOR_DIFFUSION = 2e-07


def rotation(left_index, right_index, period, direction):
    phase_index = left_index * right_index % period
    angles = phase_index.astype(jnp.float32) * (2.0 * math.pi / period)
    return (jnp.cos(angles), direction * jnp.sin(angles))


def complex_matrix(size_count, direction):
    indices = jnp.arange(size_count, dtype=jnp.int32)
    cosine_part, sine_part = rotation(indices[:, None], indices[None, :], size_count, direction)
    return jnp.stack([jnp.stack([cosine_part, -sine_part]), jnp.stack([sine_part, cosine_part])])


def transform_last(values, direction):
    part_count, species, middle, length = values.shape
    leading = 64
    second = length // leading
    shaped = values.reshape(part_count, species, middle, leading, second)
    first_matrix = complex_matrix(leading, direction)
    first_pass = jnp.einsum(
        "pqka,qsmab->psmkb", first_matrix, shaped, precision=lax.Precision.HIGHEST
    )
    cosine_part, sine_part = rotation(
        jnp.arange(leading, dtype=jnp.int32)[:, None],
        jnp.arange(second, dtype=jnp.int32)[None, :],
        length,
        direction,
    )
    turned = jnp.stack(
        [
            first_pass[0] * cosine_part - first_pass[1] * sine_part,
            first_pass[0] * sine_part + first_pass[1] * cosine_part,
        ]
    )
    second_matrix = complex_matrix(second, direction)
    second_pass = jnp.einsum(
        "pqkb,qsmjb->psmkj", second_matrix, turned, precision=lax.Precision.HIGHEST
    )
    return second_pass.reshape(part_count, species, middle, length)


def signed_squares(wave_index, total):
    signed = jnp.where(2 * wave_index < total, wave_index, wave_index - total).astype(jnp.float32)
    angular = 2.0 * math.pi * signed
    return angular * angular


def section_factors(row_wave, col_wave, total_rows, total_cols):
    wave_number = signed_squares(row_wave, total_rows) + signed_squares(col_wave, total_cols)
    normalize = 1.0 / (total_rows * total_cols)
    growths = []
    forcings = []
    for diffusion, decay_rate in (
        (SUBSTRATE_DIFFUSION, FEED_RATE),
        (ACTIVATOR_DIFFUSION, FEED_RATE + KILL_RATE),
    ):
        linear = -diffusion * wave_number - decay_rate
        exponent = linear * (0.5 * TIME_STEP)
        growths.append(jnp.exp(exponent) * normalize)
        forcings.append(jnp.expm1(exponent) / linear * normalize)
    return (jnp.stack(growths), jnp.stack(forcings))


def advance(spectra, growth, forcing):
    real_part = spectra[0]
    imag_part = spectra[1]
    return jnp.stack(
        [growth * real_part + forcing * imag_part, growth * imag_part - forcing * real_part]
    )


def col_forward(values):
    return lax.all_to_all(values, "col", split_axis=2, concat_axis=3, tiled=True)


def col_backward(values):
    return lax.all_to_all(values, "col", split_axis=3, concat_axis=2, tiled=True)


def row_forward(values):
    return lax.all_to_all(values, "row", split_axis=2, concat_axis=3, tiled=True)


def row_backward(values):
    return lax.all_to_all(values, "row", split_axis=3, concat_axis=2, tiled=True)


def on_device(substrate, activator):
    row_count, col_count = substrate.shape
    total_rows = row_count * lax.axis_size("row")
    total_cols = col_count * lax.axis_size("col")
    row_index = lax.axis_index("row")
    col_index = lax.axis_index("col")
    reaction = substrate * activator * activator
    fields = jnp.stack(
        [jnp.stack([substrate, activator]), jnp.stack([FEED_RATE - reaction, reaction])]
    )
    spectra = transform_last(col_forward(fields), -1)
    spectra = row_forward(col_forward(jnp.swapaxes(spectra, 2, 3)))
    spectra = transform_last(spectra, -1)
    local_cols = col_count // lax.axis_size("row")
    col_wave = (
        col_count * col_index
        + local_cols * row_index
        + jnp.arange(local_cols, dtype=jnp.int32)[:, None]
    )
    row_wave = jnp.arange(total_rows, dtype=jnp.int32)[None, :]
    growth, forcing = section_factors(row_wave, col_wave, total_rows, total_cols)
    spectra = transform_last(advance(spectra, growth, forcing), 1)
    spectra = col_backward(row_backward(spectra))
    spectra = jnp.swapaxes(spectra, 2, 3)
    spectra = transform_last(spectra, 1)
    fields = lax.all_to_all(spectra[:1], "col", split_axis=3, concat_axis=2, tiled=True)
    return (fields[0, 0], fields[0, 1])


MESH = pl.DeviceIdType.MESH
LANES = 128


def split(values):
    high = values.astype(jnp.bfloat16)
    low = (values - high.astype(jnp.float32)).astype(jnp.bfloat16)
    return high, low


def contract_last(left, right):
    return lax.dot_general(
        left, right, (((1,), (1,)), ((), ())), preferred_element_type=jnp.float32
    )


def block_transpose(pieces):
    first, second, third, fourth = pieces
    lane = lax.broadcasted_iota(jnp.int32, first.shape, 1)
    upper = lane < LANES // 2
    even = lane // (LANES // 4) % 2 == 0

    def far(a, b):
        return (
            jnp.where(upper, a, pltpu.roll(b, LANES // 2, 1)),
            jnp.where(upper, pltpu.roll(a, LANES // 2, 1), b),
        )

    def near(a, b):
        return (
            jnp.where(even, a, pltpu.roll(b, LANES // 4, 1)),
            jnp.where(even, pltpu.roll(a, 3 * LANES // 4, 1), b),
        )

    first, third = far(first, third)
    second, fourth = far(second, fourth)
    first, second = near(first, second)
    third, fourth = near(third, fourth)
    return first, second, third, fourth


def section_kernel(
    rows, cols, u_hbm, v_hbm, tables_hbm, sections, u_ref, v_ref, tables_ref,
    forth, flipped, x_in, packed, wide, filters, spectrum, send, recv, result,
    ready, load_sem, in_send, in_recv, s_send, s_recv, out_send, out_recv,
):
    devices = rows * cols
    total = u_ref.shape[1] * cols
    half = total // 2
    band = u_ref.shape[0] // cols
    quarter = band // 4
    chunk = half // 2
    group = 32
    row = lax.axis_index("row")
    col = lax.axis_index("col")
    me = row * cols + col

    loads = [
        pltpu.make_async_copy(source, target, load_sem.at[index])
        for index, (source, target) in enumerate(
            ((v_hbm, v_ref), (u_hbm, u_ref), (tables_hbm, tables_ref))
        )
    ]
    for load in loads:
        load.start()
    barrier = pltpu.get_barrier_semaphore()

    def greet(semaphore, other_row, other_col):
        pl.semaphore_signal(
            semaphore, inc=1, device_id=(other_row, other_col), device_id_type=MESH
        )

    for step in range(1, cols):
        greet(barrier, row, lax.rem(col + step, cols))
    for step in range(1, rows):
        greet(barrier, lax.rem(row + rows - step, rows), col)
    pl.semaphore_wait(barrier, rows + cols - 2)

    def in_copy(step, field):
        ref = (u_ref, v_ref)[field]
        other = lax.rem(col + step, cols)
        return pltpu.make_async_remote_copy(
            src_ref=ref.at[pl.ds(pl.multiple_of(other * band, band), band)],
            dst_ref=x_in.at[field, col],
            send_sem=in_send.at[0],
            recv_sem=in_recv.at[field],
            device_id=(row, other),
            device_id_type=MESH,
        )

    for field in (1, 0):
        loads[1 - field].wait()
        for step in range(1, cols):
            in_copy(step, field).start()
    for step in range(1, rows):
        greet(ready, lax.rem(row + step, rows), col)
    for field, ref in enumerate((u_ref, v_ref)):
        x_in[field, col] = ref[pl.ds(pl.multiple_of(col * band, band), band)]
    loads[2].wait()

    def build(target, coarse, fine):
        def body(step, carry):
            cosine = tables_ref[6 + coarse, pl.ds(step, 1)]
            sine = tables_ref[7 + coarse, pl.ds(step, 1)]
            high, low = split(cosine * tables_ref[fine] + sine * tables_ref[fine + 1])
            at = pl.ds(pl.multiple_of(step * group, group), group)
            target[0, at] = high
            target[1, at] = low
            return carry

        lax.fori_loop(0, half // group, body, 0)

    build(forth.at[0], 0, 0)
    build(forth.at[1], 0, 2)

    def wave(position):
        return jnp.where(position < half, 2 * position, 2 * (position - half) + 1)

    def fill_filters():
        shape = (band, total)
        q = wave(me * band + lax.broadcasted_iota(jnp.int32, shape, 0))
        p = wave(lax.broadcasted_iota(jnp.int32, shape, 1))
        wave_number = signed_squares(p, total) + signed_squares(q, total)
        for index, (diffusion, decay_rate) in enumerate((
            (SUBSTRATE_DIFFUSION, FEED_RATE),
            (ACTIVATOR_DIFFUSION, FEED_RATE + KILL_RATE),
        )):
            linear = -diffusion * wave_number - decay_rate
            growth = jnp.exp(linear * (0.5 * TIME_STEP))
            filters[2 * index] = growth
            filters[2 * index + 1] = (growth - 1.0) / linear

    def remote(leg, other):
        return pltpu.make_async_remote_copy(
            src_ref=send.at[leg, other],
            dst_ref=recv.at[leg, me],
            send_sem=s_send.at[0],
            recv_sem=s_recv.at[leg],
            device_id=other,
            device_id_type=pl.DeviceIdType.LOGICAL,
        )

    def all_of(source, target, send_sem, recv_sem):
        return pltpu.make_async_remote_copy(
            src_ref=source,
            dst_ref=target,
            send_sem=send_sem,
            recv_sem=recv_sem,
            device_id=(row, lax.rem(col + 1, cols)),
            device_id_type=MESH,
        )

    def arrived(leg):
        blocks = recv.at[leg, pl.ds(0, devices - 1)]
        all_of(blocks, blocks, s_send.at[0], s_recv.at[leg]).wait_recv()

    def gather(field):
        blocks = x_in.at[field, pl.ds(0, cols - 1)]
        all_of(blocks, blocks, in_send.at[0], in_recv.at[field]).wait_recv()

    def spread(parity, field):
        high, low = split(field)
        for copy_at in range(4):
            wide[parity, copy_at * band : (copy_at + 1) * band] = high
            wide[parity, (4 + copy_at) * band : (5 + copy_at) * band] = low

    def product(high, low, parity):
        both = contract_last(high, wide[parity])
        return both[:, :LANES] + both[:, LANES:] + contract_last(low, wide[parity, :LANES])

    def stage(leg, first, values):
        count = values.shape[0] // band
        lane = lax.broadcasted_iota(jnp.int32, (count, quarter, LANES), 2) // (LANES // 4)
        out = values.reshape(count, band, LANES)
        piece = out[:, :quarter]
        for j in range(1, 4):
            piece = jnp.where(lane == j, out[:, j * quarter : (j + 1) * quarter], piece)
        send[leg, pl.ds(first, count)] = piece


    def begin(leg):
        for step in range(1, devices):
            over = step - 1 if step < cols else step
            turn = (3, 1, 2, 0)[over % cols]
            other_row = lax.rem(row + over // cols, rows)
            remote(leg, other_row * cols + lax.rem(col + turn, cols)).start()
        recv[leg, me] = send[leg, me]

    def lead(leg):
        count = devices // 2
        for step in range(2):
            parity = lax.rem(me // count + 1 + step, 2)
            stage(leg, parity * count, product(forth[parity, 0], forth[parity, 1], parity))
            for k in range(step, count):
                remote(leg, parity * count + lax.rem(me + k, count)).start()
        recv[leg, me] = send[leg, me]

    def forward(leg):
        for parity in range(2):
            stage(
                leg,
                parity * (devices // 2),
                product(forth[parity, 0], forth[parity, 1], parity),
            )
        begin(leg)

    def swift(leg):
        count = devices // 4
        side = me // (2 * count)
        mine = lax.rem(me, 2 * count) // count
        for step in range(2):
            part = lax.rem(mine + 1 + step, 2)
            at = pl.ds(pl.multiple_of(part * chunk, chunk), chunk)
            first = product(forth[0, 0, at], forth[0, 1, at], 0)
            second = product(flipped[0, at], flipped[1, at], 1)
            stage(leg, part * count, first + second)
            stage(leg, part * count + 2 * count, first - second)
            for away, nearest in ((1 - side, 0), (side, step)):
                for k in range(nearest, count):
                    other = part * count + lax.rem(me + k, count)
                    remote(leg, other + 2 * count * away).start()
        recv[leg, me] = send[leg, me]

    def inverse(leg):
        count = devices // 4
        for part in range(2):
            at = slice(part * chunk, (part + 1) * chunk)
            first = product(forth[0, 0, at], forth[0, 1, at], 0)
            second = product(flipped[0, at], flipped[1, at], 1)
            stage(leg, part * count, first + second)
            stage(leg, part * count + 2 * count, first - second)
        begin(leg)

    def pack(parity, rows_at, pair):
        high, low = split(jnp.concatenate(pair, axis=0))
        at = slice(rows_at[1] * LANES, (rows_at[1] + 1) * LANES)
        first = rows_at[0] * 2 * quarter
        packed[parity, first : first + 2 * quarter, at] = high
        packed[parity, band + first : band + first + 2 * quarter, at] = low

    def turned(leg, g):
        return block_transpose([recv[leg, 4 * g + k] for k in range(4)])

    def dots(parity, high, low):
        dot = functools.partial(jnp.dot, preferred_element_type=jnp.float32)
        both = packed[parity]
        out = dot(both, high)
        return out[:band] + out[band:] + dot(both[:band], low)

    def land_forward(leg):
        arrived(leg)
        groups = devices // 8
        for g in range(groups):
            first, second = turned(leg, g), turned(leg, g + groups)
            for pair in range(2):
                a = [first[2 * pair], first[2 * pair + 1]]
                b = [second[2 * pair], second[2 * pair + 1]]
                pack(0, (pair, g), [m + n for m, n in zip(a, b)])
                pack(1, (pair, g), [m - n for m, n in zip(a, b)])
        return jnp.concatenate(
            [dots(0, forth[0, 0], forth[0, 1]), dots(1, flipped[0], flipped[1])], axis=1
        )

    def land_inverse(leg):
        arrived(leg)
        groups = devices // 8
        for parity in range(2):
            for g in range(groups):
                pieces = turned(leg, parity * groups + g)
                for pair in range(2):
                    pack(parity, (pair, g), [pieces[2 * pair], pieces[2 * pair + 1]])
        first = dots(0, forth[0, 0], forth[0, 1])
        second = dots(1, forth[1, 0], forth[1, 1])
        return first + second, first - second

    def gathered(field, start):
        return jnp.concatenate([x_in[field, start + block] for block in range(cols // 2)], axis=1)

    def spread_field(lower, upper):
        spread(0, lower + upper)
        spread(1, lower - upper)

    def halves(field):
        return gathered(field, 0), gathered(field, cols // 2)

    gather(1)
    spread_field(*halves(1))
    pl.semaphore_wait(ready, rows - 1)
    lead(0)
    gather(0)
    spread_field(*(u * v * v for u, v in zip(halves(0), halves(1))))
    forward(1)
    spread_field(*halves(0))
    forward(2)
    build(flipped, 2, 4)
    fill_filters()

    def spread_spectrum(values):
        spread(0, values[:, :half])
        spread(1, values[:, half:])

    activator = filters[2] * land_forward(0)
    reaction = land_forward(1)
    spread_spectrum(activator + filters[3] * reaction)
    spectrum[...] = filters[1] * reaction
    swift(3)
    spread_spectrum(filters[0] * land_forward(2) - spectrum[...])
    inverse(4)

    def out_copy(step, field):
        other = lax.rem(col + step, cols)
        return pltpu.make_async_remote_copy(
            src_ref=result.at[field, other],
            dst_ref=sections.at[field, pl.ds(pl.multiple_of(col * band, band), band)],
            send_sem=out_send.at[0],
            recv_sem=out_recv.at[0],
            device_id=(row, other),
            device_id_type=MESH,
        )

    for leg, field in ((3, 1), (4, 0)):
        for side, out in enumerate(land_inverse(leg)):
            for block in range(cols // 2):
                at = slice(block * half * 2 // cols, (block + 1) * half * 2 // cols)
                result[field, side * (cols // 2) + block] = out[:, at]
        for step in range(1, cols):
            out_copy(step, field).start()
        sections[field, pl.ds(pl.multiple_of(col * band, band), band)] = result[field, col]
    sent = send.at[:, pl.ds(0, devices - 1)]
    all_of(sent, sent, s_send.at[0], s_recv.at[0]).wait_send()
    sent = x_in.at[:, pl.ds(0, cols - 1)]
    all_of(sent, sent, in_send.at[0], in_recv.at[0]).wait_send()
    sent = result.at[:, pl.ds(0, cols - 1)]
    all_of(sent, sent, out_send.at[0], out_recv.at[0]).wait()


def tables(total, group):
    half = total // 2
    short, wave = np.arange(group), np.arange(half)
    coarse = np.arange(half // group) * group

    def angles(left, right):
        return 2.0 * np.pi / total * (left[:, None] * right[None, :] % total)

    parts = []
    for fine in (
        angles(2 * short, wave), angles(2 * short + 1, wave), angles(short, 2 * wave + 1)
    ):
        parts += [np.cos(fine) + np.sin(fine), np.cos(fine) - np.sin(fine)]
    for rough in (angles(2 * coarse, wave), angles(coarse, 2 * wave + 1)):
        parts += [np.cos(rough), np.sin(rough)]
    parts = [np.pad(part, ((0, group - part.shape[0]), (0, 0))) for part in parts]
    return jnp.asarray(np.stack(parts), jnp.float32)


def on_device_fused(rows, cols, substrate, activator):
    height, width = substrate.shape
    total = width * cols
    band = height // cols
    devices = rows * cols
    half = total // 2
    bf16, f32 = jnp.bfloat16, jnp.float32
    dma = pltpu.SemaphoreType.DMA
    vmem = pl.BlockSpec(memory_space=pltpu.VMEM)
    operands = (substrate, activator, tables(total, 32))
    sections = pl.pallas_call(
        functools.partial(section_kernel, rows, cols),
        out_shape=jax.ShapeDtypeStruct((2,) + substrate.shape, f32),
        in_specs=[pl.BlockSpec(memory_space=pltpu.HBM)] * 3,
        out_specs=vmem,
        scratch_shapes=[
            pltpu.VMEM(substrate.shape, f32),
            pltpu.VMEM(substrate.shape, f32),
            pltpu.VMEM((10, 32, half), f32),
            pltpu.VMEM((2, 2, half, half), bf16),
            pltpu.VMEM((2, half, half), bf16),
            pltpu.VMEM((2, cols, band, width), f32),
            pltpu.VMEM((2, 2 * band, half), bf16),
            pltpu.VMEM((2, 8 * band, half), bf16),
            pltpu.VMEM((4, band, total), f32),
            pltpu.VMEM((band, total), f32),
            pltpu.VMEM((5, devices, band // 4, LANES), f32),
            pltpu.VMEM((5, devices, band // 4, LANES), f32),
            pltpu.VMEM((2, cols, band, width), f32),
            pltpu.SemaphoreType.REGULAR,
            dma((3,)),
            dma((1,)),
            dma((2,)),
            dma((1,)),
            dma((5,)),
            dma((1,)),
            dma((1,)),
        ],
        compiler_params=pltpu.CompilerParams(
            collective_id=0, has_side_effects=True, vmem_limit_bytes=48 * 2**20
        ),
    )(*(pltpu.with_memory_space_constraint(value, pltpu.HBM) for value in operands))
    zero = -(FEED_RATE)
    constant = FEED_RATE * math.expm1(zero * 0.5 * TIME_STEP) / zero
    normalize = 1.0 / (total * total)
    return sections[0] * normalize + constant, sections[1] * normalize


def dispatch(rows, cols, substrate, activator):
    height, width = substrate.shape
    total = width * cols
    band = height // cols
    dense_fits = total * total * 4 <= 16 * 2**20
    fits = height * rows == total and 4 * band == LANES and band * rows * cols == total
    if fits and dense_fits and width == 256:
        return on_device_fused(rows, cols, substrate, activator)
    return on_device(substrate, activator)


def solution(mesh):
    in_specs = (P("row", "col"), P("row", "col"))
    out_specs = (P("row", "col"), P("row", "col"))
    return jax.shard_map(
        functools.partial(dispatch, mesh.shape["row"], mesh.shape["col"]),
        mesh=mesh,
        in_specs=in_specs,
        out_specs=out_specs,
        check_vma=False,
    )
```
